64 devices in a mesh: dp: 4 (over x, y), ep: 16 (over z, core).
Axes of the slice: x: 2, y: 2, z: 8, core: 2. Of those that a mesh axis runs over, the one named last changes fastest.
The devices are a block of a 4x4x8 slice.
Arguments:
- x_tokens: bfloat16 [4096, 2048], P(('dp', 'ep')), parts along dimension 0
- slot_expert: int32 [80], replicated
- w1_slots: bfloat16 [80, 2048, 1408], P('ep')
- w3_slots: bfloat16 [80, 2048, 1408], P('ep')
- w2_slots: bfloat16 [80, 1408, 2048], P('ep')
- assign: int32 [4096, 6], P(('dp', 'ep')), parts along dimension 0
- w_router: bfloat16 [2048, 64], replicated
- w1_shared: bfloat16 [2048, 2816], replicated
- w3_shared: bfloat16 [2048, 2816], replicated
- w2_shared: bfloat16 [2816, 2048], replicated
Outputs:
- output: bfloat16 [4096, 2048], P(('dp', 'ep')), parts along dimension 0
There are 4 independent parts. The reference program is written for one: setup_inputs(seed, part) draws one part's arguments, and reference() takes and returns one part's arrays. A program takes and returns all parts, laid end to end along the dimension named above; an argument that names none is the same for every part.
All inputs are finite; a program needn't handle non-finite values.
Results may differ from the reference program's by a relative error of at most 0.00157.
Values are sent between devices in bfloat16 or wider.
A program may use at most 768 MiB of HBM per device.

```python
import jax
import jax.numpy as jnp
from jax import lax

DIM_MODEL = 2048
FF_EXPERT = 1408
FF_SHARED = 2816
NUM_EXPERTS = 64
TOP_K = 6
NUM_SLOTS = 80
GROUP_SIZE = 16
TOK_DEV = 64

TOKENS = TOK_DEV * GROUP_SIZE
CAP_ROWS = max(4, (3 * TOK_DEV * TOP_K) // NUM_SLOTS)
SEG_ROWS = min(TOKENS, GROUP_SIZE * CAP_ROWS)
ROUTE_SCALE = 2.5


def draw_routing(key_shared, key_part):
    key_rank, key_place = jax.random.split(key_shared, 2)
    rank_expert = jax.random.permutation(key_rank, NUM_EXPERTS).astype(jnp.int32)
    base_of_slot = jax.random.permutation(key_place, NUM_SLOTS).astype(jnp.int32)
    slot_expert = rank_expert[base_of_slot % NUM_EXPERTS]
    slot_of_base = jnp.argsort(base_of_slot).astype(jnp.int32)
    key_noise, key_coin, key_pick = jax.random.split(key_part, 3)
    rank_ids = jnp.arange(NUM_EXPERTS, dtype=jnp.int32)
    rank_bias = (2 * TOP_K * 4096) // (NUM_EXPERTS * (rank_ids + 1))
    noise_int = jax.random.randint(key_noise, (TOKENS, NUM_EXPERTS), 0, 4096, dtype=jnp.int32)
    token_ids = jnp.arange(TOKENS, dtype=jnp.int32)
    forced = token_ids < CAP_ROWS
    force_bonus = jnp.where(forced[:, None] & (rank_ids[None, :] == 0), 16384, 0)
    rank_score = (noise_int + rank_bias[None, :] + force_bonus) * NUM_EXPERTS + rank_ids[None, :]
    chosen_rank = lax.top_k(rank_score, TOP_K)[1].astype(jnp.int32)
    copies = (NUM_SLOTS - 1 - chosen_rank) // NUM_EXPERTS + 1
    coin_flip = jax.random.randint(key_coin, (TOKENS, TOP_K), 0, 2, dtype=jnp.int32)
    pick_copy = jax.random.randint(key_pick, (TOKENS, TOP_K), 0, 65536, dtype=jnp.int32) % copies
    keep_first = (coin_flip == 0) | (forced[:, None] & (chosen_rank == 0))
    copy_index = jnp.where(keep_first, 0, pick_copy)
    slot_pick = slot_of_base[chosen_rank + copy_index * NUM_EXPERTS]
    device_of = (token_ids // TOK_DEV)[:, None]
    group_key = (device_of * NUM_SLOTS + slot_pick).reshape(-1)
    sort_order = jnp.argsort(group_key, stable=True)
    sorted_key = group_key[sort_order]
    first_pos = jnp.searchsorted(sorted_key, sorted_key, side='left').astype(jnp.int32)
    rank_sorted = jnp.arange(TOKENS * TOP_K, dtype=jnp.int32) - first_pos
    rank_flat = jnp.zeros((TOKENS * TOP_K,), jnp.int32).at[sort_order].set(rank_sorted)
    assign = jnp.where(rank_flat < CAP_ROWS, slot_pick.reshape(-1), -1).reshape(TOKENS, TOP_K)
    return slot_expert, assign.astype(jnp.int32)


def setup_inputs(seed: int = 0, part: int = 0) -> dict:
    weight_keys = jax.random.split(jax.random.key(seed), 8)
    part_key = jax.random.fold_in(jax.random.key(seed + 1), part)
    key_tokens, key_route = jax.random.split(part_key, 2)
    slot_expert, assign = draw_routing(weight_keys[0], key_route)
    x_tokens = jax.random.normal(key_tokens, (TOKENS, DIM_MODEL), jnp.float32)
    w1_experts = jax.random.normal(weight_keys[1], (NUM_EXPERTS, DIM_MODEL, FF_EXPERT), jnp.float32) * DIM_MODEL ** -0.5
    w3_experts = jax.random.normal(weight_keys[2], (NUM_EXPERTS, DIM_MODEL, FF_EXPERT), jnp.float32) * DIM_MODEL ** -0.5
    w2_experts = jax.random.normal(weight_keys[3], (NUM_EXPERTS, FF_EXPERT, DIM_MODEL), jnp.float32) * FF_EXPERT ** -0.5
    w_router = jax.random.normal(weight_keys[4], (DIM_MODEL, NUM_EXPERTS), jnp.float32) * DIM_MODEL ** -0.5
    w1_shared = jax.random.normal(weight_keys[5], (DIM_MODEL, FF_SHARED), jnp.float32) * DIM_MODEL ** -0.5
    w3_shared = jax.random.normal(weight_keys[6], (DIM_MODEL, FF_SHARED), jnp.float32) * DIM_MODEL ** -0.5
    w2_shared = jax.random.normal(weight_keys[7], (FF_SHARED, DIM_MODEL), jnp.float32) * FF_SHARED ** -0.5
    return {
        'x_tokens': x_tokens.astype(jnp.bfloat16),
        'slot_expert': slot_expert,
        'w1_slots': w1_experts.astype(jnp.bfloat16)[slot_expert],
        'w3_slots': w3_experts.astype(jnp.bfloat16)[slot_expert],
        'w2_slots': w2_experts.astype(jnp.bfloat16)[slot_expert],
        'assign': assign,
        'w_router': w_router.astype(jnp.bfloat16),
        'w1_shared': w1_shared.astype(jnp.bfloat16),
        'w3_shared': w3_shared.astype(jnp.bfloat16),
        'w2_shared': w2_shared.astype(jnp.bfloat16),
    }


def gate_weights(x_tokens, assign, slot_expert, w_router):
    logits = jnp.dot(x_tokens, w_router, preferred_element_type=jnp.float32)
    gate_prob = jax.nn.sigmoid(logits)
    is_kept = assign >= 0
    chosen = slot_expert[jnp.maximum(assign, 0)]
    picked = jnp.where(is_kept, jnp.take_along_axis(gate_prob, chosen, axis=1), 0.0)
    gate_total = jnp.sum(picked, axis=1, keepdims=True)
    return ROUTE_SCALE * picked / jnp.maximum(gate_total, 1e-30), is_kept


def shared_expert(x_tokens, w1_shared, w3_shared, w2_shared):
    h_gate = jnp.dot(x_tokens, w1_shared, preferred_element_type=jnp.float32)
    h_up = jnp.dot(x_tokens, w3_shared, preferred_element_type=jnp.float32)
    mid_act = (jax.nn.silu(h_gate) * h_up).astype(jnp.bfloat16)
    return jnp.dot(mid_act, w2_shared, preferred_element_type=jnp.float32)


def reference(x_tokens, slot_expert, w1_slots, w3_slots, w2_slots, assign, w_router, w1_shared, w3_shared, w2_shared):
    route_weight, is_kept = gate_weights(x_tokens, assign, slot_expert, w_router)
    shared_out = shared_expert(x_tokens, w1_shared, w3_shared, w2_shared)
    flat_slot = jnp.where(is_kept, assign, NUM_SLOTS).reshape(-1)
    sort_order = jnp.argsort(flat_slot, stable=True)
    sorted_slot = flat_slot[sort_order]
    slot_ids = jnp.arange(NUM_SLOTS, dtype=jnp.int32)
    seg_start = jnp.searchsorted(sorted_slot, slot_ids, side='left').astype(jnp.int32)
    seg_end = jnp.searchsorted(sorted_slot, slot_ids, side='right').astype(jnp.int32)
    token_list = jnp.concatenate([(sort_order // TOP_K).astype(jnp.int32), jnp.zeros((SEG_ROWS,), jnp.int32)])
    weight_list = jnp.concatenate([route_weight.reshape(-1)[sort_order], jnp.zeros((SEG_ROWS,), route_weight.dtype)])
    row_offsets = jnp.arange(SEG_ROWS, dtype=jnp.int32)

    def slot_step(acc_rows, slot_id):
        seg_begin = seg_start[slot_id]
        row_ids = lax.dynamic_slice(token_list, (seg_begin,), (SEG_ROWS,))
        row_weight = lax.dynamic_slice(weight_list, (seg_begin,), (SEG_ROWS,))
        row_weight = jnp.where(row_offsets < seg_end[slot_id] - seg_begin, row_weight, 0.0)
        x_rows = x_tokens[row_ids]
        h_gate = jnp.dot(x_rows, w1_slots[slot_id], preferred_element_type=jnp.float32)
        h_up = jnp.dot(x_rows, w3_slots[slot_id], preferred_element_type=jnp.float32)
        mid_act = (jax.nn.silu(h_gate) * h_up).astype(jnp.bfloat16)
        out_rows = jnp.dot(mid_act, w2_slots[slot_id], preferred_element_type=jnp.float32).astype(jnp.bfloat16)
        acc_rows = acc_rows.at[row_ids].add(row_weight[:, None] * out_rows.astype(jnp.float32))
        return acc_rows, None

    routed = lax.scan(slot_step, jnp.zeros((TOKENS, DIM_MODEL), jnp.float32), slot_ids)[0]
    return (shared_out + routed).astype(jnp.bfloat16)
```

```python
import functools

import jax
import jax.numpy as jnp
from jax import lax
from jax.experimental import pallas as pl
from jax.experimental.pallas import tpu as pltpu
from jax.sharding import PartitionSpec as P

ROUTE_SCALE = 2.5
MESH = pl.DeviceIdType.MESH
LANES = 128
CAP = 16
A_RING = 3
B_RING = 6
COL_CHUNKS = 4

F32 = jnp.float32
BF16 = jnp.bfloat16


def kernel(
    group, x_ref, asg_ref, se_ref, wr_ref, w1, w3, w2, v1, v3, v2, y_ref,
    xall, tall, tsend, xg, h, ob, osib, s1, r1, sn, rn, zsh, hs, wcs, abuf, bbuf,
    xs_sem, xr_sem, xds_sem, xdr_sem, ts_sem, tr_sem, tds_sem, tdr_sem,
    os_sem, or_sem, rs_sem, rr_sem, a_sem, b_sem,
):
    tok, dim = x_ref.shape
    top_k = asg_ref.shape[1]
    slots, _, ff = w1.shape
    ff_sh = v1.shape[1]
    nz = group // 2
    half_tok = tok // 2
    nc = COL_CHUNKS
    cw = dim // nc
    hw = cw // 2
    wide = -(-(ff // LANES) // 2) * LANES
    widths = (wide, ff - wide)
    sh_units = [(o, min(wide, ff_sh - o)) for o in range(0, ff_sh, wide)]
    nsu = len(sh_units)
    sh_pieces = ff_sh // ff

    me = lax.axis_index("ep")
    z = me // 2
    c = me % 2
    sib = 2 * z + (1 - c)

    def at(zz):
        return lax.rem(zz + 2 * nz, nz)

    nb = (2 * at(z + 1) + c, 2 * at(z - 1) + c)

    def remote(src, dst, ssem, rsem, dev):
        return pltpu.make_async_remote_copy(
            src_ref=src, dst_ref=dst, send_sem=ssem, recv_sem=rsem, device_id={"ep": dev}, device_id_type=MESH
        )

    def away(d, s):
        return at(z - s) if d == 0 else at(z + s)

    def a_copies(u_slot, first, second, width):
        return [
            pltpu.make_async_copy(src, abuf.at[u_slot, i, :, pl.ds(0, width)], a_sem.at[u_slot, i])
            for i, src in enumerate((first, second))
        ]

    def a_shared(u):
        off, width = sh_units[u]
        cols = pl.ds(off, width)
        return a_copies(u % A_RING, v1.at[:, cols], v3.at[:, cols], width)

    def a_routed(l, half):
        cols = pl.ds(half * wide, widths[half])
        slot = lax.rem(nsu + 2 * l + half, A_RING)
        return a_copies(slot, w1.at[l, :, cols], w3.at[l, :, cols], widths[half])

    def a_start(u):
        for cp in a_shared(u) if u < nsu else a_routed((u - nsu) // 2, (u - nsu) % 2):
            cp.start()

    nsb = sh_pieces * nc

    def b_shared(v):
        q, p = v // sh_pieces, v % sh_pieces
        return pltpu.make_async_copy(v2.at[pl.ds(p * ff, ff), pl.ds(q * cw, cw)], bbuf.at[v % B_RING], b_sem.at[v % B_RING])

    def b_routed(i):
        q, l = i // slots, i % slots
        slot = (nsb + i) % B_RING
        return pltpu.make_async_copy(w2.at[l, :, pl.ds(pl.multiple_of(q * cw, LANES), cw)], bbuf.at[slot], b_sem.at[slot])

    def b_start(v):
        (b_shared(v) if v < nsb else b_routed(v - nsb)).start()

    for u in range(A_RING):
        a_start(u)
    for v in range(B_RING):
        b_start(v)

    barrier = pltpu.get_barrier_semaphore()
    for peer in (nb[0], nb[1], sib):
        pl.semaphore_signal(barrier, inc=1, device_id={"ep": peer}, device_id_type=MESH)
    pl.semaphore_wait(barrier, 3)

    def x_part(d, m):
        return m // 2 + 1, pl.ds(((m % 2) ^ d) * half_tok, half_tok)

    def x_send(d, m):
        s, rows = x_part(d, m)
        blk = 2 * away(d, s - 1) + c
        src = x_ref.at[rows] if s == 1 else xall.at[blk, rows]
        return remote(src, xall.at[blk, rows], xs_sem.at[d, m], xr_sem.at[d, m], nb[d])

    def x_recv(d, m):
        s, rows = x_part(d, m)
        blk = 2 * away(d, s) + c
        return remote(xall.at[blk, rows], xall.at[blk, rows], xs_sem.at[d, m], xr_sem.at[d, m], nb[d])

    def x_cross(d, m, core):
        s, rows = x_part(d, m)
        blk = 2 * away(d, s) + core
        return remote(xall.at[blk, rows], xall.at[blk, rows], xds_sem.at[d * 7 + m], xdr_sem.at[d * 7 + m], sib)

    def x_cross_own(blk):
        return remote(x_ref, xall.at[blk], xds_sem.at[14], xdr_sem.at[14], sib)

    def t_send(d, m):
        blk = 2 * away(d, m) + c
        src = tsend if m == 0 else tall.at[blk]
        return remote(src, tall.at[blk], ts_sem.at[d, m], tr_sem.at[d, m], nb[d])

    def t_recv(d, m):
        blk = 2 * away(d, m + 1) + c
        return remote(tall.at[blk], tall.at[blk], ts_sem.at[d, m], tr_sem.at[d, m], nb[d])

    def t_cross(d, m, core):
        blk = 2 * away(d, m + 1) + core
        return remote(tall.at[blk], tall.at[blk], tds_sem.at[d * 4 + m], tdr_sem.at[d * 4 + m], sib)

    def t_cross_own(blk):
        return remote(tsend, tall.at[blk], tds_sem.at[7], tdr_sem.at[7], sib)

    t_last = (3, 2)

    def take_x(m):
        for d in (0, 1):
            x_recv(d, m).wait_recv()
            if m + 2 <= 6:
                x_send(d, m + 2).start()
            x_cross(d, m, c).start()

    def take_t(m):
        for d in (0, 1):
            if m <= t_last[d]:
                t_recv(d, m).wait_recv()
                if m + 1 <= t_last[d]:
                    t_send(d, m + 1).start()
                t_cross(d, m, c).start()

    for m in (0, 1):
        for d in (0, 1):
            x_send(d, m).start()
    x_cross_own(me).start()

    num_slots = se_ref.shape[1]
    num_exp = wr_ref.shape[1]
    exp_ids = lax.broadcasted_iota(jnp.int32, (num_exp, LANES), 0)
    slot_lane = jnp.concatenate([se_ref[...], jnp.full((1, LANES - num_slots), -1, jnp.int32)], axis=1)
    holds = jnp.where(exp_ids == slot_lane, 1.0, 0.0).astype(BF16)
    w_slot = jnp.dot(wr_ref[...], holds, preferred_element_type=F32).astype(BF16)
    gate = jax.nn.sigmoid(jnp.dot(x_ref[...], w_slot, preferred_element_type=F32))
    lane = lax.broadcasted_iota(jnp.int32, (tok, LANES), 1)
    asg = asg_ref[...]
    picked = [
        jnp.sum(jnp.where(lane == asg[:, k : k + 1], gate, 0.0), axis=1, keepdims=True) for k in range(top_k)
    ]
    total = functools.reduce(lambda a, b: a + b, picked)
    table = jnp.full((tok, LANES), -1.0, F32)
    for k in range(top_k):
        table = jnp.where(lane == k, asg[:, k : k + 1].astype(F32), table)
        table = jnp.where(lane == 8 + k, ROUTE_SCALE * picked[k] / jnp.maximum(total, 1e-30), table)
    table = jnp.concatenate([table, jnp.full((LANES - tok, LANES), -1.0, F32)], axis=0)
    table = jnp.transpose(table)[:16]
    tsend[...] = table
    tall[me] = table
    xall[me] = x_ref[...]

    def shared_up(u):
        for cp in a_shared(u):
            cp.wait()
        off, width = sh_units[u]
        slot = u % A_RING
        up = jnp.dot(x_ref[...], abuf[slot, 0, :, :width], preferred_element_type=F32)
        lin = jnp.dot(x_ref[...], abuf[slot, 1, :, :width], preferred_element_type=F32)
        hs[:, off : off + width] = (jax.nn.silu(up) * lin).astype(BF16)
        if u + A_RING < nsu + 2 * slots:
            a_start(u + A_RING)

    def shared_down(q):
        acc = None
        for p in range(sh_pieces):
            v = q * sh_pieces + p
            b_shared(v).wait()
            part = jnp.dot(hs[:, p * ff : (p + 1) * ff], bbuf[v % B_RING], preferred_element_type=F32)
            acc = part if acc is None else acc + part
            b_start(v + B_RING)
        zsh[:, q * cw : (q + 1) * cw] = acc

    tri = jnp.where(
        lax.broadcasted_iota(jnp.int32, (LANES, LANES), 0) < lax.broadcasted_iota(jnp.int32, (LANES, LANES), 1), 1.0, 0.0
    ).astype(BF16)
    seg = slots * CAP

    def choose(tab, rows, slot_of):
        row = lax.broadcasted_iota(jnp.int32, (rows, LANES), 0)
        want = slot_of(row // CAP).astype(F32)
        named = jnp.zeros((rows, LANES), F32)
        weight = jnp.zeros((rows, LANES), F32)
        for k in range(top_k):
            hit = tab[k : k + 1, :] == want
            named = jnp.where(hit, 1.0, named)
            weight = jnp.where(hit, tab[8 + k : 9 + k, :], weight)
        rank = jnp.dot(named.astype(BF16), tri, preferred_element_type=F32)
        return (named > 0.0) & (rank == (row % CAP).astype(F32)), weight

    def dispatch(zz):
        def one(core, _):
            j = 2 * zz + core
            mine, _w = choose(tall[j], seg, lambda i: me * slots + i)
            pick = jnp.where(mine, 1.0, 0.0).astype(BF16)[:, :tok]
            rows = jnp.dot(pick, xall[j], preferred_element_type=F32).astype(BF16)
            for l in range(slots):
                xg[l, core * nz + zz] = rows[l * CAP : (l + 1) * CAP]
            return 0

        lax.fori_loop(0, 2, one, 0)

    def weigh(zz):
        mine, weight = choose(
            tall[2 * zz + c], 2 * seg, lambda i: jnp.where(i < slots, me * slots + i, sib * slots + i - slots)
        )
        full = jnp.where(mine, weight, 0.0)
        full = jnp.concatenate([full, jnp.zeros((2 * LANES - 2 * seg, LANES), F32)], axis=0)
        full = jnp.transpose(full)[:tok]
        hi = full.astype(BF16)
        rest = full - hi.astype(F32)
        mid = rest.astype(BF16)
        low = (rest - mid.astype(F32)).astype(BF16)
        wcs[zz] = jnp.concatenate([hi, mid, low], axis=0)

    def ready(s):
        if s == 0:
            x_cross_own(sib).wait_recv()
            t_cross_own(sib).wait_recv()
            spots = (z,)
        elif s < nz // 2:
            for d in (0, 1):
                x_cross(d, 2 * s - 2, 1 - c).wait_recv()
                x_cross(d, 2 * s - 1, 1 - c).wait_recv()
                t_cross(d, s - 1, 1 - c).wait_recv()
            spots = (away(0, s), away(1, s))
        else:
            for d in (0, 1):
                x_cross(d, 2 * s - 2, 1 - c).wait_recv()
            t_cross(0, s - 1, 1 - c).wait_recv()
            spots = (away(0, s),)
        for zz in spots:
            dispatch(zz)
            weigh(zz)

    shared_up(0)
    for d in (0, 1):
        t_send(d, 0).start()
    t_cross_own(me).start()
    take_x(0)
    shared_up(1)
    take_x(1)
    take_t(0)
    shared_up(2)
    take_x(2)
    for u in range(3, nsu):
        shared_up(u)
    ready(0)
    take_x(3)
    take_t(1)
    shared_down(0)
    shared_down(1)
    ready(1)
    take_x(4)
    shared_down(2)
    shared_down(3)
    take_x(5)
    take_t(2)
    ready(2)
    take_x(6)
    take_t(3)
    ready(3)
    ready(4)

    def up_slot(l, _):
        rows = xg[l].reshape(group * CAP, dim)
        for half in (0, 1):
            for cp in a_routed(l, half):
                cp.wait()
            slot = lax.rem(nsu + 2 * l + half, A_RING)
            width = widths[half]
            both = jnp.concatenate([abuf[slot, 0, :, :width], abuf[slot, 1, :, :width]], axis=1)
            res = jnp.dot(rows, both, preferred_element_type=F32)
            h[l, :, half * wide : half * wide + width] = (jax.nn.silu(res[:, :width]) * res[:, width:]).astype(BF16)
            ahead = nsu + half + A_RING - nsu
            step, nxt = ahead // 2, ahead % 2

            @pl.when(l + step < slots)
            def _():
                for cp in a_routed(l + step, nxt):
                    cp.start()

        return 0

    lax.fori_loop(0, slots, up_slot, 0)

    def down(q):
        def one(l, _):
            i = q * slots + l
            b_routed(i).wait()
            res = jnp.dot(h[l], bbuf[(nsb + i) % B_RING], preferred_element_type=F32).astype(BF16)
            for core in (0, 1):
                ob[q, core, l] = res[core * nz * CAP : (core + 1) * nz * CAP].reshape(nz, CAP, cw)

            @pl.when(i + B_RING < slots * nc)
            def _():
                b_routed(i + B_RING).start()

            return 0

        lax.fori_loop(0, slots, one, 0)
        o_cross(q).start()

    def o_cross(q):
        return remote(ob.at[q, 1 - c], osib.at[q], os_sem.at[q], or_sem.at[q], sib)

    def partial(zz, q):
        rhs = jnp.concatenate([ob[q, c, :, zz].reshape(seg, cw), osib[q, :, zz].reshape(seg, cw)], axis=0)
        res = jnp.dot(wcs[zz][:, : 2 * seg], rhs, preferred_element_type=F32)
        return res[:tok] + res[tok : 2 * tok] + res[2 * tok :]

    def r_copy(d, q, s):
        src, dst = (s1.at[d, q], r1.at[d, q]) if s == 1 else (sn.at[d, q, s - 2], rn.at[d, q, s - 2])
        return remote(src, dst, rs_sem.at[d, q, s - 1], rr_sem.at[d, q, s - 1], nb[d])

    def sums(q, s):
        if s == 1:
            o_cross(q).wait_recv()
            part = partial(at(z + nz // 2), q)
            s1[0, q] = part[:, :hw]
            s1[1, q] = part[:, hw:]
        else:
            for d in (0, 1):
                part = partial(away(1 - d, nz // 2 + 1 - s), q)
                r_copy(d, q, s - 1).wait_recv()
                if s == 2:
                    lo, hi = part[:, :hw], part[:, hw:]
                    if d == 0:
                        lo = lo + r1[0, q]
                    else:
                        hi = hi + r1[1, q]
                    sn[d, q, 0, :, :hw] = lo
                    sn[d, q, 0, :, hw:] = hi
                else:
                    sn[d, q, s - 2] = part + rn[d, q, s - 3]
        for d in (0, 1):
            r_copy(d, q, s).start()

    def finish(q):
        part = partial(z, q) + zsh[:, q * cw : (q + 1) * cw]
        for d in (0, 1):
            r_copy(d, q, 4).wait_recv()
        y_ref[:, q * cw : (q + 1) * cw] = (part + rn[0, q, 2] + rn[1, q, 2]).astype(y_ref.dtype)

    down(0)
    down(1)
    sums(0, 1)
    down(2)
    sums(0, 2)
    sums(1, 1)
    down(3)
    sums(2, 1)
    sums(1, 2)
    sums(3, 1)
    sums(0, 3)
    sums(2, 2)
    sums(1, 3)
    sums(3, 2)
    sums(2, 3)
    sums(0, 4)
    sums(3, 3)
    sums(1, 4)
    sums(2, 4)
    sums(3, 4)
    for q in range(nc):
        finish(q)

    for d in (0, 1):
        for m in range(7):
            x_send(d, m).wait_send()
            x_cross(d, m, c).wait_send()
        for m in range(t_last[d] + 1):
            t_send(d, m).wait_send()
            t_cross(d, m, c).wait_send()
        for q in range(nc):
            for s in (1, 2, 3, 4):
                r_copy(d, q, s).wait_send()
    x_cross_own(me).wait_send()
    t_cross_own(me).wait_send()
    for q in range(nc):
        o_cross(q).wait_send()


def solution(mesh):
    group = mesh.shape["ep"]

    def device_step(x, slot_expert, w1, w3, w2, assign, w_router, v1, v3, v2):
        tok, dim = x.shape
        slots, _, ff = w1.shape
        nz = group // 2
        nc = COL_CHUNKS
        cw = dim // nc
        wide = -(-(ff // LANES) // 2) * LANES
        vmem = pl.BlockSpec(memory_space=pltpu.VMEM)
        hbm = pl.BlockSpec(memory_space=pl.ANY)
        dma = pltpu.SemaphoreType.DMA
        return pl.pallas_call(
            functools.partial(kernel, group),
            out_shape=jax.ShapeDtypeStruct((tok, dim), BF16),
            in_specs=[vmem] * 4 + [hbm] * 6,
            out_specs=vmem,
            scratch_shapes=[
                pltpu.VMEM((group, tok, dim), BF16),
                pltpu.VMEM((group, 16, LANES), F32),
                pltpu.VMEM((16, LANES), F32),
                pltpu.VMEM((slots, group, CAP, dim), BF16),
                pltpu.VMEM((slots, group * CAP, ff), BF16),
                pltpu.VMEM((nc, 2, slots, nz, CAP, cw), BF16),
                pltpu.VMEM((nc, slots, nz, CAP, cw), BF16),
                pltpu.VMEM((2, nc, tok, cw // 2), F32),
                pltpu.VMEM((2, nc, tok, cw // 2), F32),
                pltpu.VMEM((2, nc, 3, tok, cw), F32),
                pltpu.VMEM((2, nc, 3, tok, cw), F32),
                pltpu.VMEM((tok, dim), F32),
                pltpu.VMEM((tok, v1.shape[1]), BF16),
                pltpu.VMEM((nz, 3 * tok, 2 * LANES), BF16),
                pltpu.VMEM((A_RING, 2, dim, wide), BF16),
                pltpu.VMEM((B_RING, ff, cw), BF16),
                dma((2, 7)), dma((2, 7)), dma((15,)), dma((15,)),
                dma((2, 4)), dma((2, 4)), dma((8,)), dma((8,)),
                dma((nc,)), dma((nc,)), dma((2, nc, 4)), dma((2, nc, 4)),
                dma((A_RING, 2)), dma((B_RING,)),
            ],
            compiler_params=pltpu.CompilerParams(
                collective_id=0, has_side_effects=True, vmem_limit_bytes=66 * 1000 * 1000
            ),
            name="moe_step",
        )(x, assign, slot_expert.reshape(1, -1), w_router, w1, w3, w2, v1, v3, v2)

    token_spec = P(("dp", "ep"), None)
    slot_spec = P("ep", None, None)
    return jax.shard_map(
        device_step,
        mesh=mesh,
        in_specs=(token_spec, P(), slot_spec, slot_spec, slot_spec, token_spec, P(), P(), P(), P()),
        out_specs=token_spec,
        check_vma=False,
    )
```

```python
import functools

import jax
import jax.numpy as jnp
from jax import lax
from jax.experimental import pallas as pl
from jax.experimental.pallas import tpu as pltpu
from jax.sharding import PartitionSpec as P

ROUTE_SCALE = 2.5
MESH = pl.DeviceIdType.MESH
LANES = 128
CAP = 16
PARTS = 3
K_BLOCKS = 4
A_RING = 18
B_RING = 5
SUB = 256
CHUNKS = 4
EARLY = 2

F32 = jnp.float32
BF16 = jnp.bfloat16


def widths_of(ff):
    wide = -(-(ff // LANES) // PARTS) * LANES
    return wide, [min(wide, ff - t * wide) for t in range(PARTS)]


def kernel(
    group, x_hbm, asg_ref, se_ref, wr_ref, w1, w3, w2, v1, v3, v2, y_hbm,
    xall, tall, tsend, xg, h, ob, osib, s1, r1, sn, rn, yacc, yst, hs, wcs,
    abuf, bbuf,
    xs_sem, xr_sem, xds_sem, xdr_sem, ts_sem, tr_sem, tds_sem, tdr_sem,
    os_sem, or_sem, rs_sem, rr_sem, a_sem, b_sem, x_sem, y_sem,
):
    tok, dim = x_hbm.shape
    top_k = asg_ref.shape[0]
    slots, _, ff = w1.shape
    ff_sh = v1.shape[1]
    nz = group // 2
    far = nz // 2
    cw = dim // CHUNKS
    hw = cw // 2
    piece = tok // 2
    early = 2 * far - 3
    wide, widths = widths_of(ff)
    seg = slots * CAP
    rows_k = dim // K_BLOCKS
    per_slot = 2 * K_BLOCKS
    sh_pieces = ff_sh // ff
    nsb = CHUNKS * slots
    last_b = CHUNKS * (slots + sh_pieces)

    me = lax.axis_index("ep")
    z = me // 2
    c = me % 2
    sib = 2 * z + (1 - c)

    def at(zz):
        return lax.rem(zz + 2 * nz, nz)

    nb = (2 * at(z + 1) + c, 2 * at(z - 1) + c)

    def away(d, s):
        return at(z - s) if d == 0 else at(z + s)

    order = [(0, 0)] + [(d, s) for s in range(1, far) for d in (0, 1)] + [(0, far)]

    def chip(r):
        return away(*order[r])

    def remote(src, dst, ssem, rsem, dev):
        return pltpu.make_async_remote_copy(
            src_ref=src, dst_ref=dst, send_sem=ssem, recv_sem=rsem, device_id={"ep": dev}, device_id_type=MESH
        )

    def a_place(p, j):
        return lax.rem(per_slot * p + j, A_RING)

    def a_copy(p, j):
        rows = pl.ds(j // 2 * rows_k, rows_k)
        if isinstance(p, int) and p < sh_pieces:
            src = (v1, v3)[j % 2].at[rows, pl.ds(p * ff, ff)]
        else:
            src = (w1, w3)[j % 2].at[p - sh_pieces, rows, :]
        return pltpu.make_async_copy(src, abuf.at[a_place(p, j)], a_sem.at[a_place(p, j)])

    def a_wait(p):
        for j in range(per_slot):
            a_copy(p, j).wait()

    def a_ahead(p):
        for j in range(per_slot):
            nxt, to = (j + A_RING) % per_slot, p + (j + A_RING) // per_slot
            pl.when(to < sh_pieces + slots)(lambda: a_copy(to, nxt).start())

    def b_copy(i):
        l = i % slots
        cols = pl.ds(pl.multiple_of(i // slots * cw, LANES), cw)
        slot = i % B_RING
        return pltpu.make_async_copy(w2.at[l, :, cols], bbuf.at[slot], b_sem.at[slot])

    def b_shared(v):
        q, p = v // sh_pieces, v % sh_pieces
        slot = (nsb + v) % B_RING
        return pltpu.make_async_copy(v2.at[pl.ds(p * ff, ff), pl.ds(q * cw, cw)], bbuf.at[slot], b_sem.at[slot])

    def b_first(v):
        return b_copy(v) if v < nsb else b_shared(v - nsb)

    x_own = pltpu.make_async_copy(x_hbm, xall.at[c, z], x_sem)
    x_own.start()

    barrier = pltpu.get_barrier_semaphore()
    for peer in (nb[0], nb[1], sib):
        pl.semaphore_signal(barrier, inc=1, device_id={"ep": peer}, device_id_type=MESH)

    x_own.wait()
    for n in range(per_slot):
        a_copy(0, n).start()
    x_mine = xall[c, z]

    def gates():
        num_slots = se_ref.shape[1]
        num_exp = wr_ref.shape[0]
        exp_ids = lax.broadcasted_iota(jnp.int32, (LANES, LANES), 0)
        slot_lane = jnp.concatenate([se_ref[...], jnp.full((1, LANES - num_slots), -1, jnp.int32)], axis=1)
        holds = jnp.transpose(jnp.where(exp_ids == slot_lane, 1.0, 0.0))[:, :num_exp].astype(BF16)
        w_slot = jnp.dot(holds, wr_ref[...], preferred_element_type=F32).astype(BF16)
        gate = jax.nn.sigmoid(
            lax.dot_general(w_slot, x_mine, (((1,), (1,)), ((), ())), preferred_element_type=F32)
        )
        slot_ids = lax.broadcasted_iota(jnp.int32, (LANES, tok), 0)
        picked = [
            jnp.sum(jnp.where(slot_ids == asg_ref[k : k + 1, :], gate, 0.0), axis=0, keepdims=True)
            for k in range(top_k)
        ]
        total = functools.reduce(lambda a, b: a + b, picked)
        tsend[...] = jnp.full((16, LANES), -1.0, F32)
        for k in range(top_k):
            tsend[k : k + 1, :tok] = asg_ref[k : k + 1, :].astype(F32)
            tsend[8 + k : 9 + k, :tok] = ROUTE_SCALE * picked[k] / jnp.maximum(total, 1e-30)
        tall[c, z] = tsend[...]

    gates()
    pl.semaphore_wait(barrier, 3)

    def start_weights():
        for n in range(per_slot, A_RING):
            a_copy(n // per_slot, n % per_slot).start()
        for v in range(B_RING):
            b_first(v).start()


    def x_rows(d, m):
        return pl.ds(((m % 2) ^ d) * piece, piece)

    def x_send(d, m):
        ref = xall.at[c, away(d, m // 2), x_rows(d, m)]
        return remote(ref, ref, xs_sem.at[d, m], xr_sem.at[d, m], nb[d])

    def x_recv(d, m):
        ref = xall.at[c, away(d, m // 2 + 1), x_rows(d, m)]
        return remote(ref, ref, xs_sem.at[d, m], xr_sem.at[d, m], nb[d])

    def x_cross(d, m, core):
        ref = xall.at[core, away(d, m // 2 + 1), x_rows(d, m)]
        return remote(ref, ref, xds_sem.at[d, m], xdr_sem.at[d, m], sib)

    def x_cross_own(core):
        return remote(xall.at[core, z], xall.at[core, z], xds_sem.at[0, 7], xdr_sem.at[0, 7], sib)

    def t_send(d, m):
        src = tsend if m == 0 else tall.at[c, away(d, m)]
        return remote(src, tall.at[c, away(d, m)], ts_sem.at[d, m], tr_sem.at[d, m], nb[d])

    def t_recv(d, m):
        ref = tall.at[c, away(d, m + 1)]
        return remote(ref, ref, ts_sem.at[d, m], tr_sem.at[d, m], nb[d])

    def t_cross(d, m, core):
        ref = tall.at[core, away(d, m + 1)]
        return remote(ref, ref, tds_sem.at[d, m], tdr_sem.at[d, m], sib)

    def t_cross_own(core):
        return remote(tsend, tall.at[core, z], tds_sem.at[1, far - 1], tdr_sem.at[1, far - 1], sib)

    t_last = (far - 1, far - 2)
    x_last = 2 * far - 2

    def first_x():
        for m in (0, 1):
            for d in (0, 1):
                x_send(d, m).start()
                if m == 0:
                    t_send(d, 0).start()

    def take_x(m):
        for d in (0, 1):
            x_recv(d, m).wait_recv()
            if m + 2 <= x_last:
                x_send(d, m + 2).start()
            x_cross(d, m, c).start()

    def take_t(m):
        for d in (0, 1):
            if m <= t_last[d]:
                t_recv(d, m).wait_recv()
                if m + 1 <= t_last[d]:
                    t_send(d, m + 1).start()
                t_cross(d, m, c).start()

    tri = jnp.where(
        lax.broadcasted_iota(jnp.int32, (LANES, LANES), 0) < lax.broadcasted_iota(jnp.int32, (LANES, LANES), 1), 1.0, 0.0
    ).astype(BF16)

    def choose(tab, rows, slot_of):
        row = lax.broadcasted_iota(jnp.int32, (rows, LANES), 0)
        want = slot_of(row // CAP).astype(F32)
        named = jnp.zeros((rows, LANES), F32)
        weight = jnp.zeros((rows, LANES), F32)
        for k in range(top_k):
            hit = tab[k : k + 1, :] == want
            named = jnp.where(hit, 1.0, named)
            weight = jnp.where(hit, tab[8 + k : 9 + k, :], weight)
        rank = jnp.dot(named.astype(BF16), tri, preferred_element_type=F32)
        return (named > 0.0) & (rank == (row % CAP).astype(F32)), weight

    def dispatch(r, core):
        mine, _ = choose(tall[core, chip(r)], seg, lambda i: me * slots + i)
        pick = jnp.where(mine, 1.0, 0.0).astype(BF16)[:, :tok]
        rows = jnp.dot(pick, xall[core, chip(r)], preferred_element_type=F32).astype(BF16)
        for l in range(slots):
            xg[l, r, core] = rows[l * CAP : (l + 1) * CAP]

    def weigh(r):
        mine, weight = choose(
            tall[c, chip(r)], 2 * seg, lambda i: jnp.where(i < slots, me * slots + i, sib * slots + i - slots)
        )
        full = jnp.where(mine, weight, 0.0)
        full = jnp.concatenate([full, jnp.zeros((2 * LANES - 2 * seg, LANES), F32)], axis=0)
        full = jnp.transpose(full)[:tok]
        hi = full.astype(BF16)
        rest = full - hi.astype(F32)
        mid = rest.astype(BF16)
        low = (rest - mid.astype(F32)).astype(BF16)
        wcs[r] = jnp.concatenate([hi, mid, low], axis=0)

    def spots(s):
        return [r for r, (_, dist) in enumerate(order) if dist == s]

    def ready(s):
        if s == 0:
            t_cross_own(1 - c).wait_recv()
        else:
            for d in (0, 1):
                x_cross(d, 2 * s - 2, 1 - c).wait_recv()
                if s < far:
                    x_cross(d, 2 * s - 1, 1 - c).wait_recv()
                if s - 1 <= t_last[d]:
                    t_cross(d, s - 1, 1 - c).wait_recv()
        for r in spots(s):
            for core in (0, 1):
                dispatch(r, core)

    def weights_of(s):
        for r in spots(s):
            weigh(r)

    def gated(rows, p, t, put):
        end = t * wide + widths[t]
        for off in range(t * wide, end, SUB):
            width = min(SUB, end - off)
            cols = slice(off, off + width)

            def weight(w):
                return jnp.concatenate([abuf[a_place(p, 2 * kb + w), :, cols] for kb in range(K_BLOCKS)], axis=0)

            both = jnp.concatenate([weight(0), weight(1)], axis=1)
            res = jnp.dot(rows, both, preferred_element_type=F32)
            put(off, width, (jax.nn.silu(res[:, :width]) * res[:, width:]).astype(BF16))

    def shared_up(n):
        p, t = n // PARTS, n % PARTS
        if t == 0:
            a_wait(p)

        def put(off, width, val):
            hs[:, p * ff + off : p * ff + off + width] = val

        gated(x_mine, p, t, put)
        if t == PARTS - 1:
            for j in range(per_slot):
                a_copy(p + (j + A_RING) // per_slot, (j + A_RING) % per_slot).start()

    def shared_down(q):
        acc = None
        for p in range(sh_pieces):
            v = q * sh_pieces + p
            b_shared(v).wait()
            part = jnp.dot(hs[:, p * ff : (p + 1) * ff], bbuf[(nsb + v) % B_RING], preferred_element_type=F32)
            acc = part if acc is None else acc + part
            if nsb + v + B_RING < last_b:
                b_first(nsb + v + B_RING).start()
        yacc[q] = yacc[q] + acc

    def up_rows(l, first, last):
        rows = xg[l, first:last].reshape(2 * (last - first) * CAP, dim)
        lo, hi = 2 * first * CAP, 2 * last * CAP

        def put(off, width, val):
            h[l, lo:hi, off : off + width] = val

        for t in range(PARTS):
            gated(rows, l + sh_pieces, t, put)

    def up_near(l):
        a_wait(l + sh_pieces)
        up_rows(l, 0, early)

    def up_far():
        def one(l, _):
            up_rows(l, early, nz)
            a_ahead(l + sh_pieces)
            return 0

        lax.fori_loop(0, EARLY, one, 0)

    def up_all():
        def one(l, _):
            a_wait(l + sh_pieces)
            up_rows(l, 0, nz)
            a_ahead(l + sh_pieces)
            return 0

        lax.fori_loop(EARLY, slots, one, 0)

    def o_cross(q):
        return remote(ob.at[q % 2, :, :, 1 - c], osib.at[q], os_sem.at[q], or_sem.at[q], sib)

    def down(q, hooks):
        if q >= 2:
            o_cross(q - 2).wait_send()

        def one(l, _):
            i = q * slots + l
            b_copy(i).wait()
            res = jnp.dot(h[l], bbuf[i % B_RING], preferred_element_type=F32).astype(BF16)
            ob[q % 2, l] = res.reshape(nz, 2, CAP, cw)

            @pl.when(i + B_RING < nsb)
            def _():
                b_copy(i + B_RING).start()

            for hl, fn in hooks.items():
                pl.when(l == hl)(fn)
            return 0

        lax.fori_loop(0, slots, one, 0)
        o_cross(q).start()
        if q == CHUNKS - 1:
            for v in range(B_RING):
                b_first(nsb + v).start()

    def r_copy(d, k, s):
        src, dst = (s1.at[d, k], r1.at[d, k]) if s == 1 else (sn.at[d, k, s - 2], rn.at[d, k, s - 2])
        return remote(src, dst, rs_sem.at[d, k, s - 1], rr_sem.at[d, k, s - 1], nb[d])

    def partial(k, r):
        rhs = jnp.concatenate([ob[k % 2, :, r, c].reshape(seg, cw), osib[k, :, r].reshape(seg, cw)], axis=0)
        res = jnp.dot(wcs[r][:, : 2 * seg], rhs, preferred_element_type=F32)
        return res[:tok] + res[tok : 2 * tok] + res[2 * tok :]

    def partials(k):
        o_cross(k).wait_recv()
        part = partial(k, nz - 1)
        s1[0, k] = part[:, :hw]
        s1[1, k] = part[:, hw:]
        for s in range(2, far + 1):
            for d in (0, 1):
                sn[d, k, s - 2] = partial(k, order.index((1 - d, far + 1 - s)))
            if s == 2:
                for d in (0, 1):
                    r_copy(d, k, 1).start()
        yacc[k] = partial(k, 0)

    def step(k, s):
        for d in (0, 1):
            r_copy(d, k, s - 1).wait_recv()
            if s == 2:
                cols = slice(0, hw) if d == 0 else slice(hw, cw)
                sn[d, k, 0, :, cols] = sn[d, k, 0, :, cols] + r1[d, k]
            else:
                sn[d, k, s - 2] = sn[d, k, s - 2] + rn[d, k, s - 3]
            r_copy(d, k, s).start()

    def y_out(q):
        return pltpu.make_async_copy(yst.at[q], y_hbm.at[:, pl.ds(q * cw, cw)], y_sem.at[q])

    def finish(k):
        for d in (0, 1):
            r_copy(d, k, far).wait_recv()
        yst[k] = (yacc[k] + rn[0, k, far - 2] + rn[1, k, far - 2]).astype(BF16)
        y_out(k).start()

    x_cross_own(c).start()
    t_cross_own(c).start()
    first_x()
    start_weights()
    shared_up(0)
    take_x(0)
    take_t(0)
    shared_up(1)
    shared_up(2)
    x_cross_own(1 - c).wait_recv()
    ready(0)
    take_x(1)
    weights_of(0)
    shared_up(3)
    take_x(2)
    take_t(1)
    shared_up(4)
    shared_up(5)
    ready(1)
    take_x(3)
    weights_of(1)
    take_x(4)
    take_t(2)
    ready(2)
    up_near(0)
    take_x(5)
    take_t(3)
    up_near(1)
    take_x(6)
    weights_of(2)
    ready(3)
    weights_of(3)
    weights_of(4)
    ready(4)
    up_far()
    up_all()
    down(0, {})
    down(1, {1: lambda: partials(0)})
    down(2, {1: lambda: partials(1), 4: lambda: step(0, 2)})
    down(3, {1: lambda: partials(2), 3: lambda: step(1, 2)})
    step(0, 3)
    partials(3)
    step(2, 2)
    step(1, 3)
    step(3, 2)
    shared_down(0)
    step(0, 4)
    shared_down(1)
    step(2, 3)
    shared_down(2)
    step(1, 4)
    shared_down(3)
    step(3, 3)
    finish(0)
    step(2, 4)
    finish(1)
    step(3, 4)
    finish(2)
    finish(3)

    for d in (0, 1):
        for m in range(x_last + 1):
            x_send(d, m).wait_send()
            x_cross(d, m, c).wait_send()
        for m in range(t_last[d] + 1):
            t_send(d, m).wait_send()
            t_cross(d, m, c).wait_send()
        for k in range(CHUNKS):
            for s in range(1, far + 1):
                r_copy(d, k, s).wait_send()
    x_cross_own(c).wait_send()
    t_cross_own(c).wait_send()
    for k in (CHUNKS - 2, CHUNKS - 1):
        o_cross(k).wait_send()
    for q in range(CHUNKS):
        y_out(q).wait()


def solution(mesh):
    group = mesh.shape["ep"]

    def device_step(x, slot_expert, w1, w3, w2, assign, w_router, v1, v3, v2):
        tok, dim = x.shape
        slots, _, ff = w1.shape
        nz = group // 2
        far = nz // 2
        cw = dim // CHUNKS
        vmem = pl.BlockSpec(memory_space=pltpu.VMEM)
        hbm = pl.BlockSpec(memory_space=pl.ANY)
        dma = pltpu.SemaphoreType.DMA
        return pl.pallas_call(
            functools.partial(kernel, group),
            out_shape=jax.ShapeDtypeStruct((tok, dim), BF16),
            in_specs=[hbm] + [vmem] * 3 + [hbm] * 6,
            out_specs=hbm,
            scratch_shapes=[
                pltpu.VMEM((2, nz, tok, dim), BF16),
                pltpu.VMEM((2, nz, 16, LANES), F32),
                pltpu.VMEM((16, LANES), F32),
                pltpu.VMEM((slots, nz, 2, CAP, dim), BF16),
                pltpu.VMEM((slots, nz * 2 * CAP, ff), BF16),
                pltpu.VMEM((2, slots, nz, 2, CAP, cw), BF16),
                pltpu.VMEM((CHUNKS, slots, nz, CAP, cw), BF16),
                pltpu.VMEM((2, CHUNKS, tok, cw // 2), F32),
                pltpu.VMEM((2, CHUNKS, tok, cw // 2), F32),
                pltpu.VMEM((2, CHUNKS, far - 1, tok, cw), F32),
                pltpu.VMEM((2, CHUNKS, far - 1, tok, cw), F32),
                pltpu.VMEM((CHUNKS, tok, cw), F32),
                pltpu.VMEM((CHUNKS, tok, cw), BF16),
                pltpu.VMEM((tok, v1.shape[1]), BF16),
                pltpu.VMEM((nz, 3 * tok, 2 * LANES), BF16),
                pltpu.VMEM((A_RING, dim // K_BLOCKS, ff), BF16),
                pltpu.VMEM((B_RING, ff, cw), BF16),
                dma((2, 8)), dma((2, 8)), dma((2, 8)), dma((2, 8)),
                dma((2, far)), dma((2, far)), dma((2, far)), dma((2, far)),
                dma((CHUNKS,)), dma((CHUNKS,)), dma((2, CHUNKS, far)), dma((2, CHUNKS, far)),
                dma((A_RING,)), dma((B_RING,)), dma(()), dma((CHUNKS,)),
            ],
            compiler_params=pltpu.CompilerParams(
                collective_id=0, has_side_effects=True, vmem_limit_bytes=67_000_000
            ),
            name="moe_step",
        )(x, assign.T, slot_expert.reshape(1, -1), w_router.T, w1, w3, w2, v1, v3, v2)

    token_spec = P(("dp", "ep"), None)
    slot_spec = P("ep", None, None)
    return jax.shard_map(
        device_step,
        mesh=mesh,
        in_specs=(token_spec, P(), slot_spec, slot_spec, slot_spec, token_spec, P(), P(), P(), P()),
        out_specs=token_spec,
        check_vma=False,
    )
```

```python
import functools

import jax
import jax.numpy as jnp
from jax import lax
from jax.experimental import pallas as pl
from jax.experimental.pallas import tpu as pltpu
from jax.sharding import PartitionSpec as P

ROUTE_SCALE = 2.5
MESH = pl.DeviceIdType.MESH
LANES = 128
CAP = 16
PARTS = 3
K_BLOCKS = 4
A_RING = 18
B_RING = 5
SUB = 512
CHUNKS = 4
UNITS = 2 * CHUNKS
EARLY = 2

F32 = jnp.float32
BF16 = jnp.bfloat16


def widths_of(ff):
    wide = -(-(ff // LANES) // PARTS) * LANES
    return wide, [min(wide, ff - t * wide) for t in range(PARTS)]


def kernel(
    group, x_hbm, asg_hbm, se_hbm, wr_hbm, w1, w3, w2, v1, v3, v2, y_hbm,
    asg_ref, se_ref, wr_ref, xall, tall, tsend, xg, h, ob, osib, s1, r1, sn, rn, yacc, yst, hs, wcs,
    abuf, bbuf,
    xs_sem, xr_sem, xds_sem, xdr_sem, ts_sem, tr_sem, tds_sem, tdr_sem,
    os_sem, or_sem, rs_sem, rr_sem, a_sem, b_sem, x_sem, g_sem, y_sem,
):
    tok, dim = x_hbm.shape
    top_k = asg_hbm.shape[0]
    slots, _, ff = w1.shape
    ff_sh = v1.shape[1]
    nz = group // 2
    far = nz // 2
    cw = dim // CHUNKS
    uw = dim // UNITS
    hw = uw // 2
    piece = tok // 2
    early = 2 * far - 3
    wide, widths = widths_of(ff)
    seg = slots * CAP
    rows_k = dim // K_BLOCKS
    per_slot = 2 * K_BLOCKS
    sh_pieces = ff_sh // ff
    nsb = CHUNKS * slots
    last_b = CHUNKS * (slots + sh_pieces)

    me = lax.axis_index("ep")
    z = me // 2
    c = me % 2
    sib = 2 * z + (1 - c)

    def at(zz):
        return lax.rem(zz + 2 * nz, nz)

    nb = (2 * at(z + 1) + c, 2 * at(z - 1) + c)

    def away(d, s):
        return at(z - s) if d == 0 else at(z + s)

    order = [(0, 0)] + [(d, s) for s in range(1, far) for d in (0, 1)] + [(0, far)]

    def chip(r):
        return away(*order[r])

    def remote(src, dst, ssem, rsem, dev):
        return pltpu.make_async_remote_copy(
            src_ref=src, dst_ref=dst, send_sem=ssem, recv_sem=rsem, device_id={"ep": dev}, device_id_type=MESH
        )

    def a_place(p, j):
        return lax.rem(per_slot * p + j, A_RING)

    def a_copy(p, j):
        rows = pl.ds(j // 2 * rows_k, rows_k)
        if isinstance(p, int) and p < sh_pieces:
            src = (v1, v3)[j % 2].at[rows, pl.ds(p * ff, ff)]
        else:
            src = (w1, w3)[j % 2].at[p - sh_pieces, rows, :]
        return pltpu.make_async_copy(src, abuf.at[a_place(p, j)], a_sem.at[a_place(p, j)])

    def a_wait(p):
        for j in range(per_slot):
            a_copy(p, j).wait()

    def a_ahead(p):
        for j in range(per_slot):
            nxt, to = (j + A_RING) % per_slot, p + (j + A_RING) // per_slot
            pl.when(to < sh_pieces + slots)(lambda: a_copy(to, nxt).start())

    def b_copy(i):
        l = i % slots
        cols = pl.ds(pl.multiple_of(i // slots * cw, LANES), cw)
        slot = i % B_RING
        return pltpu.make_async_copy(w2.at[l, :, cols], bbuf.at[slot], b_sem.at[slot])

    def b_shared(v):
        q, p = v // sh_pieces, v % sh_pieces
        slot = (nsb + v) % B_RING
        return pltpu.make_async_copy(v2.at[pl.ds(p * ff, ff), pl.ds(q * cw, cw)], bbuf.at[slot], b_sem.at[slot])

    def b_first(v):
        return b_copy(v) if v < nsb else b_shared(v - nsb)

    x_own = pltpu.make_async_copy(x_hbm, xall.at[c, z], x_sem)
    x_own.start()
    gate_copies = [
        pltpu.make_async_copy(src, dst, g_sem.at[i])
        for i, (src, dst) in enumerate(((asg_hbm, asg_ref), (se_hbm, se_ref), (wr_hbm, wr_ref)))
    ]
    for cp in gate_copies:
        cp.start()

    barrier = pltpu.get_barrier_semaphore()
    for peer in (nb[0], nb[1], sib):
        pl.semaphore_signal(barrier, inc=1, device_id={"ep": peer}, device_id_type=MESH)

    x_own.wait()
    for n in range(per_slot):
        a_copy(0, n).start()
    x_mine = xall[c, z]

    def gates():
        for cp in gate_copies:
            cp.wait()
        num_slots = se_ref.shape[1]
        num_exp = wr_ref.shape[0]
        exp_ids = lax.broadcasted_iota(jnp.int32, (LANES, LANES), 0)
        slot_lane = jnp.concatenate([se_ref[...], jnp.full((1, LANES - num_slots), -1, jnp.int32)], axis=1)
        holds = jnp.transpose(jnp.where(exp_ids == slot_lane, 1.0, 0.0))[:, :num_exp].astype(BF16)
        w_slot = jnp.dot(holds, wr_ref[...], preferred_element_type=F32).astype(BF16)
        gate = jax.nn.sigmoid(
            lax.dot_general(w_slot, x_mine, (((1,), (1,)), ((), ())), preferred_element_type=F32)
        )
        slot_ids = lax.broadcasted_iota(jnp.int32, (LANES, tok), 0)
        picked = [
            jnp.sum(jnp.where(slot_ids == asg_ref[k : k + 1, :], gate, 0.0), axis=0, keepdims=True)
            for k in range(top_k)
        ]
        total = functools.reduce(lambda a, b: a + b, picked)
        tsend[...] = jnp.full((16, LANES), -1.0, F32)
        for k in range(top_k):
            tsend[k : k + 1, :tok] = asg_ref[k : k + 1, :].astype(F32)
            tsend[8 + k : 9 + k, :tok] = ROUTE_SCALE * picked[k] / jnp.maximum(total, 1e-30)
        tall[c, z] = tsend[...]

    pl.semaphore_wait(barrier, 3)

    def start_weights():
        for n in range(per_slot, A_RING):
            a_copy(n // per_slot, n % per_slot).start()
        for v in range(B_RING):
            b_first(v).start()


    def x_rows(d, m):
        return pl.ds(((m % 2) ^ d) * piece, piece)

    def x_send(d, m):
        ref = xall.at[c, away(d, m // 2), x_rows(d, m)]
        return remote(ref, ref, xs_sem.at[d, m], xr_sem.at[d, m], nb[d])

    def x_recv(d, m):
        ref = xall.at[c, away(d, m // 2 + 1), x_rows(d, m)]
        return remote(ref, ref, xs_sem.at[d, m], xr_sem.at[d, m], nb[d])

    def x_cross(d, m, core):
        ref = xall.at[core, away(d, m // 2 + 1), x_rows(d, m)]
        return remote(ref, ref, xds_sem.at[d, m], xdr_sem.at[d, m], sib)

    def x_cross_own(core):
        return remote(xall.at[core, z], xall.at[core, z], xds_sem.at[0, 7], xdr_sem.at[0, 7], sib)

    def t_send(d, m):
        src = tsend if m == 0 else tall.at[c, away(d, m)]
        return remote(src, tall.at[c, away(d, m)], ts_sem.at[d, m], tr_sem.at[d, m], nb[d])

    def t_recv(d, m):
        ref = tall.at[c, away(d, m + 1)]
        return remote(ref, ref, ts_sem.at[d, m], tr_sem.at[d, m], nb[d])

    def t_cross(d, m, core):
        ref = tall.at[core, away(d, m + 1)]
        return remote(ref, ref, tds_sem.at[d, m], tdr_sem.at[d, m], sib)

    def t_cross_own(core):
        return remote(tsend, tall.at[core, z], tds_sem.at[1, far - 1], tdr_sem.at[1, far - 1], sib)

    t_last = (far - 1, far - 2)
    x_last = 2 * far - 2

    def first_x(m):
        for d in (0, 1):
            x_send(d, m).start()

    def take_x(m):
        for d in (0, 1):
            x_recv(d, m).wait_recv()
            if m + 2 <= x_last:
                x_send(d, m + 2).start()
            x_cross(d, m, c).start()

    def take_t(m):
        for d in (0, 1):
            if m <= t_last[d]:
                t_recv(d, m).wait_recv()
                if m + 1 <= t_last[d]:
                    t_send(d, m + 1).start()
                t_cross(d, m, c).start()

    tri = jnp.where(
        lax.broadcasted_iota(jnp.int32, (LANES, LANES), 0) < lax.broadcasted_iota(jnp.int32, (LANES, LANES), 1), 1.0, 0.0
    ).astype(BF16)

    def choose(tab, rows, slot_of):
        row = lax.broadcasted_iota(jnp.int32, (rows, LANES), 0)
        want = slot_of(row // CAP).astype(F32)
        named = jnp.zeros((rows, LANES), F32)
        weight = jnp.zeros((rows, LANES), F32)
        for k in range(top_k):
            hit = tab[k : k + 1, :] == want
            named = jnp.where(hit, 1.0, named)
            weight = jnp.where(hit, tab[8 + k : 9 + k, :], weight)
        rank = jnp.dot(named.astype(BF16), tri, preferred_element_type=F32)
        return (named > 0.0) & (rank == (row % CAP).astype(F32)), weight

    def dispatch(blocks):
        picks = []
        for r, core in blocks:
            mine, _ = choose(tall[core, chip(r)], seg, lambda i: me * slots + i)
            picks.append(jnp.where(mine, 1.0, 0.0).astype(BF16)[:, :tok])

        def one(i, _):
            cols = pl.ds(pl.multiple_of(i * cw, LANES), cw)
            for (r, core), pick in zip(blocks, picks):
                rows = jnp.dot(pick, xall[core, chip(r), :, cols], preferred_element_type=F32).astype(BF16)
                for l in range(slots):
                    xg[l, r, core, :, cols] = rows[l * CAP : (l + 1) * CAP]
            return 0

        lax.fori_loop(0, CHUNKS, one, 0)

    def weigh(r):
        mine, weight = choose(
            tall[c, chip(r)], 2 * seg, lambda i: jnp.where(i < slots, me * slots + i, sib * slots + i - slots)
        )
        full = jnp.where(mine, weight, 0.0)
        full = jnp.concatenate([full, jnp.zeros((2 * LANES - 2 * seg, LANES), F32)], axis=0)
        full = jnp.transpose(full)[:tok]
        hi = full.astype(BF16)
        rest = full - hi.astype(F32)
        mid = rest.astype(BF16)
        low = (rest - mid.astype(F32)).astype(BF16)
        wcs[r] = jnp.concatenate([hi, mid, low], axis=0)

    def spots(s):
        return [r for r, (_, dist) in enumerate(order) if dist == s]

    def ready(s):
        if s == 0:
            t_cross_own(1 - c).wait_recv()
        else:
            for d in (0, 1):
                x_cross(d, 2 * s - 2, 1 - c).wait_recv()
                if s < far:
                    x_cross(d, 2 * s - 1, 1 - c).wait_recv()
                if s - 1 <= t_last[d]:
                    t_cross(d, s - 1, 1 - c).wait_recv()
        dispatch([(r, core) for r in spots(s) for core in (0, 1)])

    def weights_of(s):
        for r in spots(s):
            weigh(r)

    def gated(rows, p, t, put):
        end = t * wide + widths[t]
        for off in range(t * wide, end, SUB):
            width = min(SUB, end - off)
            cols = slice(off, off + width)

            def weight(w):
                return jnp.concatenate([abuf[a_place(p, 2 * kb + w), :, cols] for kb in range(K_BLOCKS)], axis=0)

            both = jnp.concatenate([weight(0), weight(1)], axis=1)
            res = jnp.dot(rows, both, preferred_element_type=F32)
            put(off, width, (jax.nn.silu(res[:, :width]) * res[:, width:]).astype(BF16))

    def shared_up(n):
        p, t = n // PARTS, n % PARTS
        if t == 0:
            a_wait(p)

        def put(off, width, val):
            hs[:, p * ff + off : p * ff + off + width] = val

        gated(x_mine, p, t, put)
        if t == PARTS - 1:
            for j in range(per_slot):
                a_copy(p + (j + A_RING) // per_slot, (j + A_RING) % per_slot).start()

    def shared_down(q):
        acc = None
        for p in range(sh_pieces):
            v = q * sh_pieces + p
            b_shared(v).wait()
            part = jnp.dot(hs[:, p * ff : (p + 1) * ff], bbuf[(nsb + v) % B_RING], preferred_element_type=F32)
            acc = part if acc is None else acc + part
            if nsb + v + B_RING < last_b:
                b_first(nsb + v + B_RING).start()
        yacc[q] = yacc[q] + acc

    def up_rows(l, first, last):
        rows = xg[l, first:last].reshape(2 * (last - first) * CAP, dim)
        lo, hi = 2 * first * CAP, 2 * last * CAP

        def put(off, width, val):
            h[l, lo:hi, off : off + width] = val

        for t in range(PARTS):
            gated(rows, l + sh_pieces, t, put)

    def up_near(l):
        a_wait(l + sh_pieces)
        up_rows(l, 0, early)

    def up_far():
        def one(l, _):
            up_rows(l, early, nz)
            a_ahead(l + sh_pieces)
            return 0

        lax.fori_loop(0, EARLY, one, 0)

    def up_all():
        def one(l, _):
            a_wait(l + sh_pieces)
            up_rows(l, 0, nz)
            a_ahead(l + sh_pieces)
            return 0

        lax.fori_loop(EARLY, slots, one, 0)

    def o_cross(q, l):
        return remote(ob.at[q % 2, l, :, 1 - c], osib.at[q, l], os_sem.at[q, l], or_sem.at[q, l], sib)

    def down(q, hooks):
        if q >= 2:
            for l in range(slots):
                o_cross(q - 2, l).wait_send()

        def one(l, _):
            i = q * slots + l
            b_copy(i).wait()
            res = jnp.dot(h[l], bbuf[i % B_RING], preferred_element_type=F32).astype(BF16)
            ob[q % 2, l] = res.reshape(nz, 2, CAP, cw)
            o_cross(q, l).start()

            @pl.when(i + B_RING < nsb)
            def _():
                b_copy(i + B_RING).start()

            for hl, fn in hooks.items():
                pl.when(l == hl)(fn)
            return 0

        lax.fori_loop(0, slots, one, 0)
        if q == CHUNKS - 1:
            for v in range(B_RING):
                b_first(nsb + v).start()

    def r_copy(d, k, s):
        src, dst = (s1.at[d, k], r1.at[d, k]) if s == 1 else (sn.at[d, k, s - 2], rn.at[d, k, s - 2])
        return remote(src, dst, rs_sem.at[d, k, s - 1], rr_sem.at[d, k, s - 1], nb[d])

    def partial(k, r):
        rhs = jnp.concatenate([ob[k % 2, :, r, c].reshape(seg, cw), osib[k, :, r].reshape(seg, cw)], axis=0)
        res = jnp.dot(wcs[r][:, : 2 * seg], rhs, preferred_element_type=F32)
        return res[:tok] + res[tok : 2 * tok] + res[2 * tok :]

    def partials(k):
        for l in range(slots):
            o_cross(k, l).wait_recv()
        part = partial(k, nz - 1)
        for u in (0, 1):
            s1[0, 2 * k + u] = part[:, u * uw : u * uw + hw]
            s1[1, 2 * k + u] = part[:, u * uw + hw : (u + 1) * uw]
        for s in range(2, far + 1):
            for d in (0, 1):
                part = partial(k, order.index((1 - d, far + 1 - s)))
                for u in (0, 1):
                    sn[d, 2 * k + u, s - 2] = part[:, u * uw : (u + 1) * uw]
            if s == 2:
                for u in (0, 1):
                    for d in (0, 1):
                        r_copy(d, 2 * k + u, 1).start()
        yacc[k] = partial(k, 0)

    def step(u, s):
        for d in (0, 1):
            r_copy(d, u, s - 1).wait_recv()
            if s == 2:
                cols = slice(0, hw) if d == 0 else slice(hw, uw)
                sn[d, u, 0, :, cols] = sn[d, u, 0, :, cols] + r1[d, u]
            else:
                sn[d, u, s - 2] = sn[d, u, s - 2] + rn[d, u, s - 3]
            r_copy(d, u, s).start()

    def y_out(u):
        return pltpu.make_async_copy(yst.at[u], y_hbm.at[:, pl.ds(u * uw, uw)], y_sem.at[u])

    def finish(u):
        mine = yacc[u // 2, :, u % 2 * uw : (u % 2 + 1) * uw]
        for d in (0, 1):
            r_copy(d, u, far).wait_recv()
        yst[u] = (mine + rn[0, u, far - 2] + rn[1, u, far - 2]).astype(BF16)
        y_out(u).start()

    x_cross_own(c).start()
    first_x(0)
    gates()
    for d in (0, 1):
        t_send(d, 0).start()
    t_cross_own(c).start()
    first_x(1)
    start_weights()
    shared_up(0)
    take_x(0)
    take_t(0)
    shared_up(1)
    shared_up(2)
    take_x(1)
    x_cross_own(1 - c).wait_recv()
    ready(0)
    weights_of(0)
    shared_up(3)
    take_x(2)
    take_t(1)
    shared_up(4)
    shared_up(5)
    take_x(3)
    ready(1)
    weights_of(1)
    weights_of(2)
    take_x(4)
    take_t(2)
    ready(2)
    up_near(0)
    take_x(5)
    up_near(1)
    weights_of(3)
    take_x(6)
    take_t(3)
    ready(3)
    weights_of(4)
    ready(4)
    up_far()
    up_all()
    down(0, {})
    down(1, {1: lambda: partials(0)})
    down(2, {0: lambda: partials(1), 1: lambda: step(0, 2), 2: lambda: step(1, 2)})
    down(3, {0: lambda: [step(2, 2), step(3, 2), partials(2)] and None, 1: lambda: step(0, 3), 2: lambda: step(1, 3)})
    partials(3)
    step(4, 2)
    step(5, 2)
    step(2, 3)
    step(3, 3)
    step(0, 4)
    step(1, 4)
    step(6, 2)
    step(7, 2)
    shared_down(0)
    step(4, 3)
    step(5, 3)
    shared_down(1)
    step(2, 4)
    step(3, 4)
    shared_down(2)
    step(6, 3)
    step(7, 3)
    shared_down(3)
    step(4, 4)
    step(5, 4)
    finish(0)
    finish(1)
    step(6, 4)
    step(7, 4)
    for u in range(2, UNITS):
        finish(u)

    for d in (0, 1):
        for m in range(x_last + 1):
            x_send(d, m).wait_send()
            x_cross(d, m, c).wait_send()
        for m in range(t_last[d] + 1):
            t_send(d, m).wait_send()
            t_cross(d, m, c).wait_send()
        for k in range(UNITS):
            for s in range(1, far + 1):
                r_copy(d, k, s).wait_send()
    x_cross_own(c).wait_send()
    t_cross_own(c).wait_send()
    for k in (CHUNKS - 2, CHUNKS - 1):
        for l in range(slots):
            o_cross(k, l).wait_send()
    for u in range(UNITS):
        y_out(u).wait()


def solution(mesh):
    group = mesh.shape["ep"]

    def device_step(x, slot_expert, w1, w3, w2, assign, w_router, v1, v3, v2):
        tok, dim = x.shape
        slots, _, ff = w1.shape
        nz = group // 2
        far = nz // 2
        cw, uw = dim // CHUNKS, dim // UNITS
        hbm = pl.BlockSpec(memory_space=pl.ANY)
        dma = pltpu.SemaphoreType.DMA
        return pl.pallas_call(
            functools.partial(kernel, group),
            out_shape=jax.ShapeDtypeStruct((tok, dim), BF16),
            in_specs=[hbm] * 10,
            out_specs=hbm,
            scratch_shapes=[
                pltpu.VMEM((assign.shape[1], tok), jnp.int32),
                pltpu.VMEM((1, slot_expert.shape[0]), jnp.int32),
                pltpu.VMEM((w_router.shape[1], dim), BF16),
                pltpu.VMEM((2, nz, tok, dim), BF16),
                pltpu.VMEM((2, nz, 16, LANES), F32),
                pltpu.VMEM((16, LANES), F32),
                pltpu.VMEM((slots, nz, 2, CAP, dim), BF16),
                pltpu.VMEM((slots, nz * 2 * CAP, ff), BF16),
                pltpu.VMEM((2, slots, nz, 2, CAP, cw), BF16),
                pltpu.VMEM((CHUNKS, slots, nz, CAP, cw), BF16),
                pltpu.VMEM((2, UNITS, tok, uw // 2), F32),
                pltpu.VMEM((2, UNITS, tok, uw // 2), F32),
                pltpu.VMEM((2, UNITS, far - 1, tok, uw), F32),
                pltpu.VMEM((2, UNITS, far - 1, tok, uw), F32),
                pltpu.VMEM((CHUNKS, tok, cw), F32),
                pltpu.VMEM((UNITS, tok, uw), BF16),
                pltpu.VMEM((tok, v1.shape[1]), BF16),
                pltpu.VMEM((nz, 3 * tok, 2 * LANES), BF16),
                pltpu.VMEM((A_RING, dim // K_BLOCKS, ff), BF16),
                pltpu.VMEM((B_RING, ff, cw), BF16),
                dma((2, 8)), dma((2, 8)), dma((2, 8)), dma((2, 8)),
                dma((2, far)), dma((2, far)), dma((2, far)), dma((2, far)),
                dma((CHUNKS, slots)), dma((CHUNKS, slots)), dma((2, UNITS, far)), dma((2, UNITS, far)),
                dma((A_RING,)), dma((B_RING,)), dma(()), dma((3,)), dma((UNITS,)),
            ],
            compiler_params=pltpu.CompilerParams(
                collective_id=0, has_side_effects=True, vmem_limit_bytes=67_000_000
            ),
            name="moe_step",
        )(x, assign.T, slot_expert.reshape(1, -1), w_router.T, w1, w3, w2, v1, v3, v2)

    token_spec = P(("dp", "ep"), None)
    slot_spec = P("ep", None, None)
    return jax.shard_map(
        device_step,
        mesh=mesh,
        in_specs=(token_spec, P(), slot_spec, slot_spec, slot_spec, token_spec, P(), P(), P(), P()),
        out_specs=token_spec,
        check_vma=False,
    )
```

```python
import functools

import jax
import jax.numpy as jnp
from jax import lax
from jax.experimental import pallas as pl
from jax.experimental.pallas import tpu as pltpu
from jax.sharding import PartitionSpec as P

ROUTE_SCALE = 2.5
MESH = pl.DeviceIdType.MESH
LANES = 128
CAP = 16
PARTS = 3
K_BLOCKS = 4
A_RING = 18
B_RING = 5
SUB = 512
CHUNKS = 4
UNITS = 2 * CHUNKS
EARLY = 2

F32 = jnp.float32
BF16 = jnp.bfloat16


def widths_of(ff):
    wide = -(-(ff // LANES) // PARTS) * LANES
    return wide, [min(wide, ff - t * wide) for t in range(PARTS)]


def kernel(
    group, x_hbm, asg_hbm, se_hbm, wr_hbm, w1, w3, w2, v1, v3, v2, y_hbm,
    asg_ref, se_ref, wr_ref, xall, tall, tsend, xg, h, ob, osib, s1, r1, sn, rn, yacc, yst, hs, wcs,
    abuf, bbuf,
    xs_sem, xr_sem, xds_sem, xdr_sem, ts_sem, tr_sem, tds_sem, tdr_sem,
    os_sem, or_sem, rs_sem, rr_sem, a_sem, b_sem, x_sem, g_sem, y_sem,
):
    tok, dim = x_hbm.shape
    top_k = asg_hbm.shape[0]
    slots, _, ff = w1.shape
    ff_sh = v1.shape[1]
    nz = group // 2
    far = nz // 2
    cw = dim // CHUNKS
    uw = dim // UNITS
    hw = uw // 2
    piece = tok // 2
    early = 2 * far - 3
    wide, widths = widths_of(ff)
    seg = slots * CAP
    rows_k = dim // K_BLOCKS
    per_slot = 2 * K_BLOCKS
    sh_pieces = ff_sh // ff
    nsb = CHUNKS * slots
    last_b = CHUNKS * (slots + sh_pieces)

    me = lax.axis_index("ep")
    z = me // 2
    c = me % 2
    sib = 2 * z + (1 - c)

    def at(zz):
        return lax.rem(zz + 2 * nz, nz)

    nb = (2 * at(z + 1) + c, 2 * at(z - 1) + c)

    def away(d, s):
        return at(z - s) if d == 0 else at(z + s)

    order = [(0, 0)] + [(d, s) for s in range(1, far) for d in (0, 1)] + [(0, far)]

    def chip(r):
        return away(*order[r])

    def remote(src, dst, ssem, rsem, dev):
        return pltpu.make_async_remote_copy(
            src_ref=src, dst_ref=dst, send_sem=ssem, recv_sem=rsem, device_id={"ep": dev}, device_id_type=MESH
        )

    def a_place(p, j):
        return lax.rem(per_slot * p + j, A_RING)

    def a_copy(p, j):
        rows = pl.ds(j // 2 * rows_k, rows_k)
        if isinstance(p, int) and p < sh_pieces:
            src = (v1, v3)[j % 2].at[rows, pl.ds(p * ff, ff)]
        else:
            src = (w1, w3)[j % 2].at[p - sh_pieces, rows, :]
        return pltpu.make_async_copy(src, abuf.at[a_place(p, j)], a_sem.at[a_place(p, j)])

    def a_wait(p):
        for j in range(per_slot):
            a_copy(p, j).wait()

    def a_ahead(p):
        for j in range(per_slot):
            nxt, to = (j + A_RING) % per_slot, p + (j + A_RING) // per_slot
            pl.when(to < sh_pieces + slots)(lambda: a_copy(to, nxt).start())

    def b_copy(i):
        l = i % slots
        cols = pl.ds(pl.multiple_of(i // slots * cw, LANES), cw)
        slot = i % B_RING
        return pltpu.make_async_copy(w2.at[l, :, cols], bbuf.at[slot], b_sem.at[slot])

    def b_shared(v):
        q, p = v // sh_pieces, v % sh_pieces
        slot = (nsb + v) % B_RING
        return pltpu.make_async_copy(v2.at[pl.ds(p * ff, ff), pl.ds(q * cw, cw)], bbuf.at[slot], b_sem.at[slot])

    def b_first(v):
        return b_copy(v) if v < nsb else b_shared(v - nsb)

    x_own = pltpu.make_async_copy(x_hbm, xall.at[c, z], x_sem)
    x_own.start()
    gate_copies = [
        pltpu.make_async_copy(src, dst, g_sem.at[i])
        for i, (src, dst) in enumerate(((asg_hbm, asg_ref), (se_hbm, se_ref), (wr_hbm, wr_ref)))
    ]
    for cp in gate_copies:
        cp.start()

    barrier = pltpu.get_barrier_semaphore()
    for peer in (nb[0], nb[1], sib):
        pl.semaphore_signal(barrier, inc=1, device_id={"ep": peer}, device_id_type=MESH)

    x_own.wait()
    for n in range(per_slot):
        a_copy(0, n).start()
    x_mine = xall[c, z]

    def gates():
        for cp in gate_copies:
            cp.wait()
        num_slots = se_ref.shape[1]
        num_exp = wr_ref.shape[0]
        exp_ids = lax.broadcasted_iota(jnp.int32, (LANES, LANES), 0)
        slot_lane = jnp.concatenate([se_ref[...], jnp.full((1, LANES - num_slots), -1, jnp.int32)], axis=1)
        holds = jnp.transpose(jnp.where(exp_ids == slot_lane, 1.0, 0.0))[:, :num_exp].astype(BF16)
        w_slot = jnp.dot(holds, wr_ref[...], preferred_element_type=F32).astype(BF16)
        gate = jax.nn.sigmoid(
            lax.dot_general(w_slot, x_mine, (((1,), (1,)), ((), ())), preferred_element_type=F32)
        )
        slot_ids = lax.broadcasted_iota(jnp.int32, (LANES, tok), 0)
        picked = [
            jnp.sum(jnp.where(slot_ids == asg_ref[k : k + 1, :], gate, 0.0), axis=0, keepdims=True)
            for k in range(top_k)
        ]
        total = functools.reduce(lambda a, b: a + b, picked)
        tsend[...] = jnp.full((16, LANES), -1.0, F32)
        for k in range(top_k):
            tsend[k : k + 1, :tok] = asg_ref[k : k + 1, :].astype(F32)
            tsend[8 + k : 9 + k, :tok] = ROUTE_SCALE * picked[k] / jnp.maximum(total, 1e-30)
        tall[c, z] = tsend[...]

    pl.semaphore_wait(barrier, 3)

    def start_weights():
        for n in range(per_slot, A_RING):
            a_copy(n // per_slot, n % per_slot).start()
        for v in range(B_RING):
            b_first(v).start()


    def x_rows(d, m):
        return pl.ds(((m % 2) ^ d) * piece, piece)

    def x_send(d, m):
        ref = xall.at[c, away(d, m // 2), x_rows(d, m)]
        return remote(ref, ref, xs_sem.at[d, m], xr_sem.at[d, m], nb[d])

    def x_recv(d, m):
        ref = xall.at[c, away(d, m // 2 + 1), x_rows(d, m)]
        return remote(ref, ref, xs_sem.at[d, m], xr_sem.at[d, m], nb[d])

    def x_cross(d, m, core):
        ref = xall.at[core, away(d, m // 2 + 1), x_rows(d, m)]
        return remote(ref, ref, xds_sem.at[d, m], xdr_sem.at[d, m], sib)

    def x_cross_own(core):
        return remote(xall.at[core, z], xall.at[core, z], xds_sem.at[0, 7], xdr_sem.at[0, 7], sib)

    def t_send(d, m):
        src = tsend if m == 0 else tall.at[c, away(d, m)]
        return remote(src, tall.at[c, away(d, m)], ts_sem.at[d, m], tr_sem.at[d, m], nb[d])

    def t_recv(d, m):
        ref = tall.at[c, away(d, m + 1)]
        return remote(ref, ref, ts_sem.at[d, m], tr_sem.at[d, m], nb[d])

    def t_cross(d, m, core):
        ref = tall.at[core, away(d, m + 1)]
        return remote(ref, ref, tds_sem.at[d, m], tdr_sem.at[d, m], sib)

    def t_cross_own(core):
        return remote(tsend, tall.at[core, z], tds_sem.at[1, far - 1], tdr_sem.at[1, far - 1], sib)

    t_last = (far - 1, far - 2)
    x_last = 2 * far - 2

    def first_x(m):
        for d in (0, 1):
            x_send(d, m).start()

    def take_x(m):
        for d in (0, 1):
            x_recv(d, m).wait_recv()
            if m + 2 <= x_last:
                x_send(d, m + 2).start()
            x_cross(d, m, c).start()

    def take_t(m):
        for d in (0, 1):
            if m <= t_last[d]:
                t_recv(d, m).wait_recv()
                if m + 1 <= t_last[d]:
                    t_send(d, m + 1).start()
                t_cross(d, m, c).start()

    tri = jnp.where(
        lax.broadcasted_iota(jnp.int32, (LANES, LANES), 0) < lax.broadcasted_iota(jnp.int32, (LANES, LANES), 1), 1.0, 0.0
    ).astype(BF16)

    def choose(tab, rows, slot_of):
        row = lax.broadcasted_iota(jnp.int32, (rows, LANES), 0)
        want = slot_of(row // CAP).astype(F32)
        named = jnp.zeros((rows, LANES), F32)
        weight = jnp.zeros((rows, LANES), F32)
        for k in range(top_k):
            hit = tab[k : k + 1, :] == want
            named = jnp.where(hit, 1.0, named)
            weight = jnp.where(hit, tab[8 + k : 9 + k, :], weight)
        rank = jnp.dot(named.astype(BF16), tri, preferred_element_type=F32)
        return (named > 0.0) & (rank == (row % CAP).astype(F32)), weight

    def dispatch(blocks):
        picks = []
        for r, core in blocks:
            mine, _ = choose(tall[core, chip(r)], seg, lambda i: me * slots + i)
            picks.append(jnp.where(mine, 1.0, 0.0).astype(BF16)[:, :tok])

        def one(i, _):
            cols = pl.ds(pl.multiple_of(i * cw, LANES), cw)
            for (r, core), pick in zip(blocks, picks):
                rows = jnp.dot(pick, xall[core, chip(r), :, cols], preferred_element_type=F32).astype(BF16)
                for l in range(slots):
                    xg[l, r, core, :, cols] = rows[l * CAP : (l + 1) * CAP]
            return 0

        lax.fori_loop(0, CHUNKS, one, 0)

    def weigh(r):
        mine, weight = choose(
            tall[c, chip(r)], 2 * seg, lambda i: jnp.where(i < slots, me * slots + i, sib * slots + i - slots)
        )
        full = jnp.where(mine, weight, 0.0)
        full = jnp.concatenate([full, jnp.zeros((2 * LANES - 2 * seg, LANES), F32)], axis=0)
        full = jnp.transpose(full)[:tok]
        hi = full.astype(BF16)
        rest = full - hi.astype(F32)
        mid = rest.astype(BF16)
        low = (rest - mid.astype(F32)).astype(BF16)
        wcs[r] = jnp.concatenate([hi, mid, low], axis=0)

    def spots(s):
        return [r for r, (_, dist) in enumerate(order) if dist == s]

    def ready(s):
        if s == 0:
            t_cross_own(1 - c).wait_recv()
        else:
            for d in (0, 1):
                x_cross(d, 2 * s - 2, 1 - c).wait_recv()
                if s < far:
                    x_cross(d, 2 * s - 1, 1 - c).wait_recv()
                if s - 1 <= t_last[d]:
                    t_cross(d, s - 1, 1 - c).wait_recv()
        dispatch([(r, core) for r in spots(s) for core in (0, 1)])

    def weights_of(s):
        for r in spots(s):
            weigh(r)

    def gated(rows, p, t, put):
        end = t * wide + widths[t]
        for off in range(t * wide, end, SUB):
            width = min(SUB, end - off)
            cols = slice(off, off + width)

            def weight(w):
                return jnp.concatenate([abuf[a_place(p, 2 * kb + w), :, cols] for kb in range(K_BLOCKS)], axis=0)

            both = jnp.concatenate([weight(0), weight(1)], axis=1)
            res = jnp.dot(rows, both, preferred_element_type=F32)
            put(off, width, (jax.nn.silu(res[:, :width]) * res[:, width:]).astype(BF16))

    def shared_up(n):
        p, t = n // PARTS, n % PARTS
        if t == 0:
            a_wait(p)

        def put(off, width, val):
            hs[:, p * ff + off : p * ff + off + width] = val

        gated(x_mine, p, t, put)
        if t == PARTS - 1:
            for j in range(per_slot):
                a_copy(p + (j + A_RING) // per_slot, (j + A_RING) % per_slot).start()

    def shared_down(q):
        acc = None
        for p in range(sh_pieces):
            v = q * sh_pieces + p
            b_shared(v).wait()
            part = jnp.dot(hs[:, p * ff : (p + 1) * ff], bbuf[(nsb + v) % B_RING], preferred_element_type=F32)
            acc = part if acc is None else acc + part
            if nsb + v + B_RING < last_b:
                b_first(nsb + v + B_RING).start()
        yacc[q] = yacc[q] + acc

    def up_rows(l, first, last):
        rows = xg[l, first:last].reshape(2 * (last - first) * CAP, dim)
        lo, hi = 2 * first * CAP, 2 * last * CAP

        def put(off, width, val):
            h[l, lo:hi, off : off + width] = val

        for t in range(PARTS):
            gated(rows, l + sh_pieces, t, put)

    def up_near(l):
        a_wait(l + sh_pieces)
        up_rows(l, 0, early)

    def up_far():
        def one(l, _):
            up_rows(l, early, nz)
            a_ahead(l + sh_pieces)
            return 0

        lax.fori_loop(0, EARLY, one, 0)

    def up_all():
        def one(l, _):
            a_wait(l + sh_pieces)
            up_rows(l, 0, nz)
            a_ahead(l + sh_pieces)
            return 0

        lax.fori_loop(EARLY, slots, one, 0)

    def o_cross(q, l):
        return remote(ob.at[q % 2, l, :, 1 - c], osib.at[q, l], os_sem.at[q, l], or_sem.at[q, l], sib)

    def down(q, hooks):
        if q >= 2:
            for l in range(slots):
                o_cross(q - 2, l).wait_send()

        for first in range(0, slots, 2):
            pair = range(first, min(first + 2, slots))
            for l in pair:
                b_copy(q * slots + l).wait()
            for l in pair:
                i = q * slots + l
                res = jnp.dot(h[l], bbuf[i % B_RING], preferred_element_type=F32).astype(BF16)
                ob[q % 2, l] = res.reshape(nz, 2, CAP, cw)
            for l in pair:
                o_cross(q, l).start()
                if q * slots + l + B_RING < nsb:
                    b_copy(q * slots + l + B_RING).start()
            for fn in hooks.get(first, ()):
                fn()
        if q == CHUNKS - 1:
            for v in range(B_RING):
                b_first(nsb + v).start()

    def r_copy(d, k, s):
        src, dst = (s1.at[d, k], r1.at[d, k]) if s == 1 else (sn.at[d, k, s - 2], rn.at[d, k, s - 2])
        return remote(src, dst, rs_sem.at[d, k, s - 1], rr_sem.at[d, k, s - 1], nb[d])

    def partial(k, r):
        rhs = jnp.concatenate([ob[k % 2, :, r, c].reshape(seg, cw), osib[k, :, r].reshape(seg, cw)], axis=0)
        res = jnp.dot(wcs[r][:, : 2 * seg], rhs, preferred_element_type=F32)
        return res[:tok] + res[tok : 2 * tok] + res[2 * tok :]

    def partials(k):
        for l in range(slots):
            o_cross(k, l).wait_recv()
        part = partial(k, nz - 1)
        for u in (0, 1):
            s1[0, 2 * k + u] = part[:, u * uw : u * uw + hw]
            s1[1, 2 * k + u] = part[:, u * uw + hw : (u + 1) * uw]
        for s in range(2, far + 1):
            for d in (0, 1):
                part = partial(k, order.index((1 - d, far + 1 - s)))
                for u in (0, 1):
                    sn[d, 2 * k + u, s - 2] = part[:, u * uw : (u + 1) * uw]
            if s == 2:
                for u in (0, 1):
                    for d in (0, 1):
                        r_copy(d, 2 * k + u, 1).start()
        yacc[k] = partial(k, 0)

    def step(u, s):
        for d in (0, 1):
            r_copy(d, u, s - 1).wait_recv()
            if s == 2:
                cols = slice(0, hw) if d == 0 else slice(hw, uw)
                sn[d, u, 0, :, cols] = sn[d, u, 0, :, cols] + r1[d, u]
            else:
                sn[d, u, s - 2] = sn[d, u, s - 2] + rn[d, u, s - 3]
            r_copy(d, u, s).start()

    def y_out(u):
        return pltpu.make_async_copy(yst.at[u], y_hbm.at[:, pl.ds(u * uw, uw)], y_sem.at[u])

    def finish(u):
        mine = yacc[u // 2, :, u % 2 * uw : (u % 2 + 1) * uw]
        for d in (0, 1):
            r_copy(d, u, far).wait_recv()
        yst[u] = (mine + rn[0, u, far - 2] + rn[1, u, far - 2]).astype(BF16)
        y_out(u).start()

    x_cross_own(c).start()
    first_x(0)
    gates()
    for d in (0, 1):
        t_send(d, 0).start()
    t_cross_own(c).start()
    first_x(1)
    start_weights()
    shared_up(0)
    take_x(0)
    take_t(0)
    shared_up(1)
    shared_up(2)
    take_x(1)
    x_cross_own(1 - c).wait_recv()
    ready(0)
    weights_of(0)
    shared_up(3)
    take_x(2)
    take_t(1)
    shared_up(4)
    shared_up(5)
    take_x(3)
    ready(1)
    weights_of(1)
    weights_of(2)
    take_x(4)
    take_t(2)
    ready(2)
    up_near(0)
    take_x(5)
    up_near(1)
    take_x(6)
    take_t(3)
    ready(3)
    ready(4)
    up_far()
    up_all()
    down(0, {})
    weights_of(3)
    weights_of(4)
    part = functools.partial
    down(1, {0: [part(partials, 0)]})
    down(2, {0: [part(step, 0, 2), part(step, 1, 2), part(partials, 1)]})
    down(3, {0: [part(step, 2, 2), part(partials, 2)], 2: [part(step, 3, 2), part(step, 0, 3)], 4: [part(step, 1, 3)]})
    partials(3)
    step(4, 2)
    step(5, 2)
    step(2, 3)
    step(3, 3)
    step(0, 4)
    step(1, 4)
    step(6, 2)
    step(7, 2)
    shared_down(0)
    step(4, 3)
    step(5, 3)
    shared_down(1)
    step(2, 4)
    step(3, 4)
    shared_down(2)
    step(6, 3)
    step(7, 3)
    shared_down(3)
    step(4, 4)
    step(5, 4)
    finish(0)
    finish(1)
    step(6, 4)
    step(7, 4)
    for u in range(2, UNITS):
        finish(u)

    for d in (0, 1):
        for m in range(x_last + 1):
            x_send(d, m).wait_send()
            x_cross(d, m, c).wait_send()
        for m in range(t_last[d] + 1):
            t_send(d, m).wait_send()
            t_cross(d, m, c).wait_send()
        for k in range(UNITS):
            for s in range(1, far + 1):
                r_copy(d, k, s).wait_send()
    x_cross_own(c).wait_send()
    t_cross_own(c).wait_send()
    for k in (CHUNKS - 2, CHUNKS - 1):
        for l in range(slots):
            o_cross(k, l).wait_send()
    for u in range(UNITS):
        y_out(u).wait()


def solution(mesh):
    group = mesh.shape["ep"]

    def device_step(x, slot_expert, w1, w3, w2, assign, w_router, v1, v3, v2):
        tok, dim = x.shape
        slots, _, ff = w1.shape
        nz = group // 2
        far = nz // 2
        cw, uw = dim // CHUNKS, dim // UNITS
        hbm = pl.BlockSpec(memory_space=pl.ANY)
        dma = pltpu.SemaphoreType.DMA
        return pl.pallas_call(
            functools.partial(kernel, group),
            out_shape=jax.ShapeDtypeStruct((tok, dim), BF16),
            in_specs=[hbm] * 10,
            out_specs=hbm,
            scratch_shapes=[
                pltpu.VMEM((assign.shape[1], tok), jnp.int32),
                pltpu.VMEM((1, slot_expert.shape[0]), jnp.int32),
                pltpu.VMEM((w_router.shape[1], dim), BF16),
                pltpu.VMEM((2, nz, tok, dim), BF16),
                pltpu.VMEM((2, nz, 16, LANES), F32),
                pltpu.VMEM((16, LANES), F32),
                pltpu.VMEM((slots, nz, 2, CAP, dim), BF16),
                pltpu.VMEM((slots, nz * 2 * CAP, ff), BF16),
                pltpu.VMEM((2, slots, nz, 2, CAP, cw), BF16),
                pltpu.VMEM((CHUNKS, slots, nz, CAP, cw), BF16),
                pltpu.VMEM((2, UNITS, tok, uw // 2), F32),
                pltpu.VMEM((2, UNITS, tok, uw // 2), F32),
                pltpu.VMEM((2, UNITS, far - 1, tok, uw), F32),
                pltpu.VMEM((2, UNITS, far - 1, tok, uw), F32),
                pltpu.VMEM((CHUNKS, tok, cw), F32),
                pltpu.VMEM((UNITS, tok, uw), BF16),
                pltpu.VMEM((tok, v1.shape[1]), BF16),
                pltpu.VMEM((nz, 3 * tok, 2 * LANES), BF16),
                pltpu.VMEM((A_RING, dim // K_BLOCKS, ff), BF16),
                pltpu.VMEM((B_RING, ff, cw), BF16),
                dma((2, 8)), dma((2, 8)), dma((2, 8)), dma((2, 8)),
                dma((2, far)), dma((2, far)), dma((2, far)), dma((2, far)),
                dma((CHUNKS, slots)), dma((CHUNKS, slots)), dma((2, UNITS, far)), dma((2, UNITS, far)),
                dma((A_RING,)), dma((B_RING,)), dma(()), dma((3,)), dma((UNITS,)),
            ],
            compiler_params=pltpu.CompilerParams(
                collective_id=0, has_side_effects=True, vmem_limit_bytes=67_000_000
            ),
            name="moe_step",
        )(x, assign.T, slot_expert.reshape(1, -1), w_router.T, w1, w3, w2, v1, v3, v2)

    token_spec = P(("dp", "ep"), None)
    slot_spec = P("ep", None, None)
    return jax.shard_map(
        device_step,
        mesh=mesh,
        in_specs=(token_spec, P(), slot_spec, slot_spec, slot_spec, token_spec, P(), P(), P(), P()),
        out_specs=token_spec,
        check_vma=False,
    )
```

```python
import functools

import jax
import jax.numpy as jnp
from jax import lax
from jax.experimental import pallas as pl
from jax.experimental.pallas import tpu as pltpu
from jax.sharding import PartitionSpec as P

ROUTE_SCALE = 2.5
MESH = pl.DeviceIdType.MESH
LANES = 128
CAP = 16
PARTS = 3
K_BLOCKS = 4
A_RING = 18
B_RING = 5
SUB = 512
CHUNKS = 4
UNITS = 2 * CHUNKS
EARLY = 2

F32 = jnp.float32
BF16 = jnp.bfloat16


def widths_of(ff):
    wide = -(-(ff // LANES) // PARTS) * LANES
    return wide, [min(wide, ff - t * wide) for t in range(PARTS)]


def kernel(
    group, x_hbm, asg_hbm, se_hbm, wr_hbm, w1, w3, w2, v1, v3, v2, y_hbm,
    asg_ref, se_ref, wr_ref, xall, tall, tsend, xg, h, ob, osib, s1, r1, sn, rn, yacc, yst, hs, wcs,
    abuf, bbuf,
    xs_sem, xr_sem, xds_sem, xdr_sem, ts_sem, tr_sem, tds_sem, tdr_sem,
    os_sem, or_sem, rs_sem, rr_sem, a_sem, b_sem, x_sem, g_sem, y_sem,
):
    tok, dim = x_hbm.shape
    top_k = asg_hbm.shape[0]
    slots, _, ff = w1.shape
    ff_sh = v1.shape[1]
    nz = group // 2
    far = nz // 2
    cw = dim // CHUNKS
    uw = dim // UNITS
    hw = uw // 2
    piece = tok // 2
    early = 2 * far - 3
    wide, widths = widths_of(ff)
    seg = slots * CAP
    rows_k = dim // K_BLOCKS
    per_slot = 2 * K_BLOCKS
    sh_pieces = ff_sh // ff
    nsb = CHUNKS * slots
    last_b = CHUNKS * (slots + sh_pieces)

    me = lax.axis_index("ep")
    z = me // 2
    c = me % 2
    sib = 2 * z + (1 - c)

    def at(zz):
        return lax.rem(zz + 2 * nz, nz)

    nb = (2 * at(z + 1) + c, 2 * at(z - 1) + c)

    def away(d, s):
        return at(z - s) if d == 0 else at(z + s)

    order = [(0, 0)] + [(d, s) for s in range(1, far) for d in (0, 1)] + [(0, far)]

    def chip(r):
        return away(*order[r])

    def remote(src, dst, ssem, rsem, dev):
        return pltpu.make_async_remote_copy(
            src_ref=src, dst_ref=dst, send_sem=ssem, recv_sem=rsem, device_id={"ep": dev}, device_id_type=MESH
        )

    def a_place(p, j):
        return lax.rem(per_slot * p + j, A_RING)

    def a_copy(p, j):
        rows = pl.ds(j // 2 * rows_k, rows_k)
        if isinstance(p, int) and p < sh_pieces:
            src = (v1, v3)[j % 2].at[rows, pl.ds(p * ff, ff)]
        else:
            src = (w1, w3)[j % 2].at[p - sh_pieces, rows, :]
        return pltpu.make_async_copy(src, abuf.at[a_place(p, j)], a_sem.at[a_place(p, j)])

    def a_wait(p):
        for j in range(per_slot):
            a_copy(p, j).wait()

    def a_ahead(p):
        for j in range(per_slot):
            nxt, to = (j + A_RING) % per_slot, p + (j + A_RING) // per_slot
            pl.when(to < sh_pieces + slots)(lambda: a_copy(to, nxt).start())

    def b_copy(i):
        l = i % slots
        cols = pl.ds(pl.multiple_of(i // slots * cw, LANES), cw)
        slot = i % B_RING
        return pltpu.make_async_copy(w2.at[l, :, cols], bbuf.at[slot], b_sem.at[slot])

    def b_shared(v):
        q, p = v // sh_pieces, v % sh_pieces
        slot = (nsb + v) % B_RING
        return pltpu.make_async_copy(v2.at[pl.ds(p * ff, ff), pl.ds(q * cw, cw)], bbuf.at[slot], b_sem.at[slot])

    def b_first(v):
        return b_copy(v) if v < nsb else b_shared(v - nsb)

    x_own = pltpu.make_async_copy(x_hbm, xall.at[c, z], x_sem)
    x_own.start()
    gate_copies = [
        pltpu.make_async_copy(src, dst, g_sem.at[i])
        for i, (src, dst) in enumerate(((asg_hbm, asg_ref), (se_hbm, se_ref), (wr_hbm, wr_ref)))
    ]
    for cp in gate_copies:
        cp.start()

    barrier = pltpu.get_barrier_semaphore()
    for peer in (nb[0], nb[1], sib):
        pl.semaphore_signal(barrier, inc=1, device_id={"ep": peer}, device_id_type=MESH)

    x_own.wait()
    for n in range(per_slot):
        a_copy(0, n).start()
    x_mine = xall[c, z]

    def gates():
        for cp in gate_copies:
            cp.wait()
        num_slots = se_ref.shape[1]
        num_exp = wr_ref.shape[0]
        exp_ids = lax.broadcasted_iota(jnp.int32, (LANES, LANES), 0)
        slot_lane = jnp.concatenate([se_ref[...], jnp.full((1, LANES - num_slots), -1, jnp.int32)], axis=1)
        holds = jnp.transpose(jnp.where(exp_ids == slot_lane, 1.0, 0.0))[:, :num_exp].astype(BF16)
        w_slot = jnp.dot(holds, wr_ref[...], preferred_element_type=F32).astype(BF16)
        gate = jax.nn.sigmoid(
            lax.dot_general(w_slot, x_mine, (((1,), (1,)), ((), ())), preferred_element_type=F32)
        )
        slot_ids = lax.broadcasted_iota(jnp.int32, (LANES, tok), 0)
        picked = [
            jnp.sum(jnp.where(slot_ids == asg_ref[k : k + 1, :], gate, 0.0), axis=0, keepdims=True)
            for k in range(top_k)
        ]
        total = functools.reduce(lambda a, b: a + b, picked)
        tsend[...] = jnp.full((16, LANES), -1.0, F32)
        for k in range(top_k):
            tsend[k : k + 1, :tok] = asg_ref[k : k + 1, :].astype(F32)
            tsend[8 + k : 9 + k, :tok] = ROUTE_SCALE * picked[k] / jnp.maximum(total, 1e-30)
        tall[c, z] = tsend[...]

    pl.semaphore_wait(barrier, 3)

    def start_weights():
        for n in range(per_slot, A_RING):
            a_copy(n // per_slot, n % per_slot).start()
        for v in range(B_RING):
            b_first(v).start()


    def x_rows(d, m):
        return pl.ds(((m % 2) ^ d) * piece, piece)

    def x_send(d, m):
        ref = xall.at[c, away(d, m // 2), x_rows(d, m)]
        return remote(ref, ref, xs_sem.at[d, m], xr_sem.at[d, m], nb[d])

    def x_recv(d, m):
        ref = xall.at[c, away(d, m // 2 + 1), x_rows(d, m)]
        return remote(ref, ref, xs_sem.at[d, m], xr_sem.at[d, m], nb[d])

    def x_cross(d, m, core):
        ref = xall.at[core, away(d, m // 2 + 1), x_rows(d, m)]
        return remote(ref, ref, xds_sem.at[d, m], xdr_sem.at[d, m], sib)

    def x_cross_own(core):
        return remote(xall.at[core, z], xall.at[core, z], xds_sem.at[0, 7], xdr_sem.at[0, 7], sib)

    def t_send(d, m):
        src = tsend if m == 0 else tall.at[c, away(d, m)]
        return remote(src, tall.at[c, away(d, m)], ts_sem.at[d, m], tr_sem.at[d, m], nb[d])

    def t_recv(d, m):
        ref = tall.at[c, away(d, m + 1)]
        return remote(ref, ref, ts_sem.at[d, m], tr_sem.at[d, m], nb[d])

    def t_cross(d, m, core):
        ref = tall.at[core, away(d, m + 1)]
        return remote(ref, ref, tds_sem.at[d, m], tdr_sem.at[d, m], sib)

    def t_cross_own(core):
        return remote(tsend, tall.at[core, z], tds_sem.at[1, far - 1], tdr_sem.at[1, far - 1], sib)

    t_last = (far - 1, far - 2)
    x_last = 2 * far - 2

    def first_x(m):
        for d in (0, 1):
            x_send(d, m).start()

    def take_x(m):
        for d in (0, 1):
            x_recv(d, m).wait_recv()
            if m + 2 <= x_last:
                x_send(d, m + 2).start()
            x_cross(d, m, c).start()

    def take_t(m):
        for d in (0, 1):
            if m <= t_last[d]:
                t_recv(d, m).wait_recv()
                if m + 1 <= t_last[d]:
                    t_send(d, m + 1).start()
                t_cross(d, m, c).start()

    tri = jnp.where(
        lax.broadcasted_iota(jnp.int32, (LANES, LANES), 0) < lax.broadcasted_iota(jnp.int32, (LANES, LANES), 1), 1.0, 0.0
    ).astype(BF16)

    def choose(tab, rows, slot_of):
        row = lax.broadcasted_iota(jnp.int32, (rows, LANES), 0)
        want = slot_of(row // CAP).astype(F32)
        named = jnp.zeros((rows, LANES), F32)
        weight = jnp.zeros((rows, LANES), F32)
        for k in range(top_k):
            hit = tab[k : k + 1, :] == want
            named = jnp.where(hit, 1.0, named)
            weight = jnp.where(hit, tab[8 + k : 9 + k, :], weight)
        rank = jnp.dot(named.astype(BF16), tri, preferred_element_type=F32)
        return (named > 0.0) & (rank == (row % CAP).astype(F32)), weight

    def dispatch(blocks):
        picks = []
        for r, core in blocks:
            mine, _ = choose(tall[core, chip(r)], seg, lambda i: me * slots + i)
            picks.append(jnp.where(mine, 1.0, 0.0).astype(BF16)[:, :tok])

        def one(i, _):
            cols = pl.ds(pl.multiple_of(i * cw, LANES), cw)
            for (r, core), pick in zip(blocks, picks):
                rows = jnp.dot(pick, xall[core, chip(r), :, cols], preferred_element_type=F32).astype(BF16)
                for l in range(slots):
                    xg[l, r, core, :, cols] = rows[l * CAP : (l + 1) * CAP]
            return 0

        lax.fori_loop(0, CHUNKS, one, 0)

    def weigh(r):
        mine, weight = choose(
            tall[c, chip(r)], 2 * seg, lambda i: jnp.where(i < slots, me * slots + i, sib * slots + i - slots)
        )
        full = jnp.where(mine, weight, 0.0)
        full = jnp.concatenate([full, jnp.zeros((2 * LANES - 2 * seg, LANES), F32)], axis=0)
        full = jnp.transpose(full)[:tok]
        hi = full.astype(BF16)
        rest = full - hi.astype(F32)
        mid = rest.astype(BF16)
        low = (rest - mid.astype(F32)).astype(BF16)
        wcs[r] = jnp.concatenate([hi, mid, low], axis=0)

    def spots(s):
        return [r for r, (_, dist) in enumerate(order) if dist == s]

    def ready(s):
        if s == 0:
            t_cross_own(1 - c).wait_recv()
        else:
            for d in (0, 1):
                x_cross(d, 2 * s - 2, 1 - c).wait_recv()
                if s < far:
                    x_cross(d, 2 * s - 1, 1 - c).wait_recv()
                if s - 1 <= t_last[d]:
                    t_cross(d, s - 1, 1 - c).wait_recv()
        dispatch([(r, core) for r in spots(s) for core in (0, 1)])

    def weights_of(s):
        for r in spots(s):
            weigh(r)

    def gated(rows, p, t, put):
        end = t * wide + widths[t]
        for off in range(t * wide, end, SUB):
            width = min(SUB, end - off)
            cols = slice(off, off + width)

            def weight(w):
                return jnp.concatenate([abuf[a_place(p, 2 * kb + w), :, cols] for kb in range(K_BLOCKS)], axis=0)

            both = jnp.concatenate([weight(0), weight(1)], axis=1)
            res = jnp.dot(rows, both, preferred_element_type=F32)
            put(off, width, (jax.nn.silu(res[:, :width]) * res[:, width:]).astype(BF16))

    def shared_up(n):
        p, t = n // PARTS, n % PARTS
        if t == 0:
            a_wait(p)

        def put(off, width, val):
            hs[:, p * ff + off : p * ff + off + width] = val

        gated(x_mine, p, t, put)
        if t == PARTS - 1:
            for j in range(per_slot):
                a_copy(p + (j + A_RING) // per_slot, (j + A_RING) % per_slot).start()

    def shared_down(q):
        acc = None
        for p in range(sh_pieces):
            v = q * sh_pieces + p
            b_shared(v).wait()
            part = jnp.dot(hs[:, p * ff : (p + 1) * ff], bbuf[(nsb + v) % B_RING], preferred_element_type=F32)
            acc = part if acc is None else acc + part
            if nsb + v + B_RING < last_b:
                b_first(nsb + v + B_RING).start()
        yacc[q] = yacc[q] + acc

    def up_rows(l, first, last):
        rows = xg[l, first:last].reshape(2 * (last - first) * CAP, dim)
        lo, hi = 2 * first * CAP, 2 * last * CAP

        def put(off, width, val):
            h[l, lo:hi, off : off + width] = val

        for t in range(PARTS):
            gated(rows, l + sh_pieces, t, put)

    def up_near(l):
        a_wait(l + sh_pieces)
        up_rows(l, 0, early)

    def up_far():
        def one(l, _):
            up_rows(l, early, nz)
            a_ahead(l + sh_pieces)
            return 0

        lax.fori_loop(0, EARLY, one, 0)

    def up_all():
        def one(l, _):
            a_wait(l + sh_pieces)
            up_rows(l, 0, nz)
            a_ahead(l + sh_pieces)
            return 0

        lax.fori_loop(EARLY, slots, one, 0)

    def o_cross(q, l):
        return remote(ob.at[q % 2, l, :, 1 - c], osib.at[q, l], os_sem.at[q, l], or_sem.at[q, l], sib)

    def down(q, hooks):
        if q >= 2:
            for l in range(slots):
                o_cross(q - 2, l).wait_send()

        for first in range(0, slots, 2):
            pair = range(first, min(first + 2, slots))
            for l in pair:
                b_copy(q * slots + l).wait()
            for l in pair:
                i = q * slots + l
                res = jnp.dot(h[l], bbuf[i % B_RING], preferred_element_type=F32).astype(BF16)
                ob[q % 2, l] = res.reshape(nz, 2, CAP, cw)
            for l in pair:
                o_cross(q, l).start()
                if q * slots + l + B_RING < nsb:
                    b_copy(q * slots + l + B_RING).start()
            for fn in hooks.get(first, ()):
                fn()
        if q == CHUNKS - 1:
            for v in range(B_RING):
                b_first(nsb + v).start()

    def r_copy(d, k, s):
        src, dst = (s1.at[d, k], r1.at[d, k]) if s == 1 else (sn.at[d, k, s - 2], rn.at[d, k, s - 2])
        return remote(src, dst, rs_sem.at[d, k, s - 1], rr_sem.at[d, k, s - 1], nb[d])

    def partial(k, r):
        rhs = jnp.concatenate([ob[k % 2, :, r, c].reshape(seg, cw), osib[k, :, r].reshape(seg, cw)], axis=0)
        res = jnp.dot(wcs[r][:, : 2 * seg], rhs, preferred_element_type=F32)
        return res[:tok] + res[tok : 2 * tok] + res[2 * tok :]

    def partials(k):
        for l in range(slots):
            o_cross(k, l).wait_recv()
        part = partial(k, nz - 1)
        for u in (0, 1):
            s1[0, 2 * k + u] = part[:, u * uw : u * uw + hw]
            s1[1, 2 * k + u] = part[:, u * uw + hw : (u + 1) * uw]
        for s in range(2, far + 1):
            for d in (0, 1):
                part = partial(k, order.index((1 - d, far + 1 - s)))
                for u in (0, 1):
                    sn[d, 2 * k + u, s - 2] = part[:, u * uw : (u + 1) * uw]
            if s == 2:
                for u in (0, 1):
                    for d in (0, 1):
                        r_copy(d, 2 * k + u, 1).start()
        yacc[k] = partial(k, 0)

    def step(u, s):
        for d in (0, 1):
            r_copy(d, u, s - 1).wait_recv()
            if s == 2:
                cols = slice(0, hw) if d == 0 else slice(hw, uw)
                sn[d, u, 0, :, cols] = sn[d, u, 0, :, cols] + r1[d, u]
            else:
                sn[d, u, s - 2] = sn[d, u, s - 2] + rn[d, u, s - 3]
            r_copy(d, u, s).start()

    def y_out(u):
        return pltpu.make_async_copy(yst.at[u], y_hbm.at[:, pl.ds(u * uw, uw)], y_sem.at[u])

    def finish(u):
        mine = yacc[u // 2, :, u % 2 * uw : (u % 2 + 1) * uw]
        for d in (0, 1):
            r_copy(d, u, far).wait_recv()
        yst[u] = (mine + rn[0, u, far - 2] + rn[1, u, far - 2]).astype(BF16)
        y_out(u).start()

    x_cross_own(c).start()
    first_x(0)
    gates()
    for d in (0, 1):
        t_send(d, 0).start()
    t_cross_own(c).start()
    first_x(1)
    start_weights()
    shared_up(0)
    take_x(0)
    take_t(0)
    shared_up(1)
    shared_up(2)
    take_x(1)
    x_cross_own(1 - c).wait_recv()
    ready(0)
    weights_of(0)
    shared_up(3)
    take_x(2)
    take_t(1)
    shared_up(4)
    shared_up(5)
    take_x(3)
    ready(1)
    ready(2)
    weights_of(1)
    weights_of(2)
    take_x(4)
    take_t(2)
    up_near(0)
    take_x(5)
    up_near(1)
    ready(3)
    take_x(6)
    take_t(3)
    weights_of(3)
    weights_of(4)
    ready(4)
    up_far()
    up_all()
    down(0, {})
    part = functools.partial
    down(1, {0: [part(partials, 0)]})
    down(2, {0: [part(partials, 1)], 2: [part(step, 0, 2), part(step, 1, 2)]})
    down(3, {0: [part(partials, 2), part(step, 2, 2), part(step, 3, 2)], 2: [part(step, 0, 3)], 4: [part(step, 1, 3)]})
    partials(3)
    step(4, 2)
    step(5, 2)
    step(2, 3)
    step(3, 3)
    step(0, 4)
    step(1, 4)
    step(6, 2)
    step(7, 2)
    shared_down(0)
    step(4, 3)
    step(5, 3)
    shared_down(1)
    step(2, 4)
    step(3, 4)
    shared_down(2)
    step(6, 3)
    step(7, 3)
    shared_down(3)
    step(4, 4)
    step(5, 4)
    finish(0)
    finish(1)
    step(6, 4)
    step(7, 4)
    for u in range(2, UNITS):
        finish(u)

    for d in (0, 1):
        for m in range(x_last + 1):
            x_send(d, m).wait_send()
            x_cross(d, m, c).wait_send()
        for m in range(t_last[d] + 1):
            t_send(d, m).wait_send()
            t_cross(d, m, c).wait_send()
        for k in range(UNITS):
            for s in range(1, far + 1):
                r_copy(d, k, s).wait_send()
    x_cross_own(c).wait_send()
    t_cross_own(c).wait_send()
    for k in (CHUNKS - 2, CHUNKS - 1):
        for l in range(slots):
            o_cross(k, l).wait_send()
    for u in range(UNITS):
        y_out(u).wait()


def solution(mesh):
    group = mesh.shape["ep"]

    def device_step(x, slot_expert, w1, w3, w2, assign, w_router, v1, v3, v2):
        tok, dim = x.shape
        slots, _, ff = w1.shape
        nz = group // 2
        far = nz // 2
        cw, uw = dim // CHUNKS, dim // UNITS
        hbm = pl.BlockSpec(memory_space=pl.ANY)
        dma = pltpu.SemaphoreType.DMA
        return pl.pallas_call(
            functools.partial(kernel, group),
            out_shape=jax.ShapeDtypeStruct((tok, dim), BF16),
            in_specs=[hbm] * 10,
            out_specs=hbm,
            scratch_shapes=[
                pltpu.VMEM((assign.shape[1], tok), jnp.int32),
                pltpu.VMEM((1, slot_expert.shape[0]), jnp.int32),
                pltpu.VMEM((w_router.shape[1], dim), BF16),
                pltpu.VMEM((2, nz, tok, dim), BF16),
                pltpu.VMEM((2, nz, 16, LANES), F32),
                pltpu.VMEM((16, LANES), F32),
                pltpu.VMEM((slots, nz, 2, CAP, dim), BF16),
                pltpu.VMEM((slots, nz * 2 * CAP, ff), BF16),
                pltpu.VMEM((2, slots, nz, 2, CAP, cw), BF16),
                pltpu.VMEM((CHUNKS, slots, nz, CAP, cw), BF16),
                pltpu.VMEM((2, UNITS, tok, uw // 2), F32),
                pltpu.VMEM((2, UNITS, tok, uw // 2), F32),
                pltpu.VMEM((2, UNITS, far - 1, tok, uw), F32),
                pltpu.VMEM((2, UNITS, far - 1, tok, uw), F32),
                pltpu.VMEM((CHUNKS, tok, cw), F32),
                pltpu.VMEM((UNITS, tok, uw), BF16),
                pltpu.VMEM((tok, v1.shape[1]), BF16),
                pltpu.VMEM((nz, 3 * tok, 2 * LANES), BF16),
                pltpu.VMEM((A_RING, dim // K_BLOCKS, ff), BF16),
                pltpu.VMEM((B_RING, ff, cw), BF16),
                dma((2, 8)), dma((2, 8)), dma((2, 8)), dma((2, 8)),
                dma((2, far)), dma((2, far)), dma((2, far)), dma((2, far)),
                dma((CHUNKS, slots)), dma((CHUNKS, slots)), dma((2, UNITS, far)), dma((2, UNITS, far)),
                dma((A_RING,)), dma((B_RING,)), dma(()), dma((3,)), dma((UNITS,)),
            ],
            compiler_params=pltpu.CompilerParams(
                collective_id=0, has_side_effects=True, vmem_limit_bytes=67_000_000
            ),
            name="moe_step",
        )(x, assign.T, slot_expert.reshape(1, -1), w_router.T, w1, w3, w2, v1, v3, v2)

    token_spec = P(("dp", "ep"), None)
    slot_spec = P("ep", None, None)
    return jax.shard_map(
        device_step,
        mesh=mesh,
        in_specs=(token_spec, P(), slot_spec, slot_spec, slot_spec, token_spec, P(), P(), P(), P()),
        out_specs=token_spec,
        check_vma=False,
    )
```
